256 devices in a mesh: scen: 4 (over x, y), lon: 64 (over z, core).
Axes of the slice: x: 2, y: 2, z: 32, core: 2. Of those that a mesh axis runs over, the one named last changes fastest.
The devices are a block of a 4x8x32 slice.
Arguments:
- tracer: float32 [32, 4, 2048, 1024], P('scen', None, 'lon'), parts along dimension 0, may hold values from 0.25 to 15, as said below
- offsets: int32 [4, 2048, 1024], P(None, 'lon'), may hold values from -12 to 12
- frac: float32 [4, 1024], replicated, may hold values from 0.02 to 0.98
- air_before: float32 [4, 2048, 1024], P(None, 'lon'), may hold values from 0.5 to 2
- air_after: float32 [4, 2048, 1024], P(None, 'lon'), may hold values from 0.05 to 15, as said below
- growth: float32 [32], P('scen'), parts along dimension 0, may hold values from 0.05 to 0.5
Outputs:
- tracer_next: float32 [32, 4, 2048, 1024], P('scen', None, 'lon'), parts along dimension 0
The draws below stay inside these ranges and needn't reach their ends.
There are 4 independent parts, one for each index of `scen`. The reference program is written for one: setup_inputs(seed, part) draws one part's arguments, and reference() takes and returns one part's arrays. A program takes and returns all parts, laid end to end along the dimension named above; an argument that names none is the same for every part. Nothing has to cross between parts.
Inputs may be any that keep to these rules, and one draw needn't show every extreme that they name: `tracer`: positive mixing ratios. `air_after`: positive air masses.
All inputs are finite; a program needn't handle non-finite values.
Results may differ from the reference program's by a relative error of at most 0.00002.
Values sent between devices are 32-bit elements; how exact they have to be, the bound alone decides.
A program may use at most 64 MiB of HBM per device.

```python
import math
import jax
import jax.numpy as jnp
from jax import lax

S = 8
LEV = 4
NLAT = 1024
OFFMAX = 12
NLON = 2048


def draw_tracer(key, part):
    shape = (S, LEV, NLON, NLAT)
    column = jnp.arange(NLON, dtype=jnp.float32) / (NLON - 1)
    base = jnp.exp(jax.random.uniform(key, shape, jnp.float32, math.log(0.3), math.log(3.0)))
    return base * (1.0 + 2.0 * column)[:, None]


def draw_air_after(key, part):
    first_key, second_key = jax.random.split(jax.random.fold_in(key, 7))
    base = jnp.exp(jax.random.uniform(first_key, (LEV, NLON, NLAT), jnp.float32, math.log(0.5), math.log(2.0)))
    banded = jnp.clip(jax.random.normal(second_key, (LEV, 1, NLAT), jnp.float32), -2.5, 2.5)
    return base * jnp.exp(0.4 * banded)


def touch_ends(drawn, key, low, top_value):
    spot = [jax.random.randint(jax.random.fold_in(key, axis), (), 0, length) for axis, length in enumerate(drawn.shape)]
    main_axis = drawn.shape.index(max(drawn.shape))
    beside = spot[:main_axis] + [(spot[main_axis] + 1) % drawn.shape[main_axis]] + spot[main_axis + 1:]
    return drawn.at[tuple(spot)].set(low).at[tuple(beside)].set(top_value)


def block_scale(rng, shape, shards, low, largest):
    gain = 1.0
    for axis_at, blocks in shards:
        heights = jax.random.uniform(jax.random.fold_in(jax.random.fold_in(rng, 6), axis_at), (blocks,), jnp.float32, low / len(shards), largest / len(shards))
        gain = gain * jnp.repeat(jnp.exp(heights), shape[axis_at] // blocks).reshape((-1,) + (1,) * (len(shape) - 1 - axis_at))
    return gain


def setup_inputs(seed: int = 0, part: int = 0) -> dict:
    arg_keys = jax.random.split(jax.random.key(seed), 7)
    part_splits = jax.random.split(jax.random.fold_in(arg_keys[6], part), 7)
    return {
        "tracer": draw_tracer(jax.random.fold_in(jax.random.fold_in(arg_keys[6], part), 71), part),
        "offsets": touch_ends(jax.random.randint(arg_keys[1], (LEV, NLON, NLAT), -OFFMAX, OFFMAX + 1), jax.random.fold_in(arg_keys[1], 1), -OFFMAX, OFFMAX).astype(jnp.int32),
        "frac": jnp.clip(jax.random.uniform(arg_keys[2], (LEV, NLAT), jnp.float32, 0.02, 0.98), 0.02, 0.98),
        "air_before": jnp.clip(jnp.exp(math.log(2.0) - 1.3862944 * jax.random.uniform(arg_keys[3], (LEV, NLON, NLAT), jnp.float32) ** block_scale(arg_keys[3], (LEV, NLON, NLAT), ((1, 64),), -0.2, 0.2)), 0.5, 2.0),
        "air_after": draw_air_after(jax.random.fold_in(arg_keys[6], 71), part),
        "growth": jnp.clip(jnp.exp(jax.random.uniform(part_splits[5], (S,), jnp.float32, math.log(0.05), math.log(0.5))), 0.05, 0.5),
    }


def cubic_weights(fraction):
    first = -fraction * (1.0 - fraction) * (2.0 - fraction) / 6.0
    second = (1.0 + fraction) * (1.0 - fraction) * (2.0 - fraction) / 2.0
    third = (1.0 + fraction) * fraction * (2.0 - fraction) / 2.0
    fourth = -(1.0 + fraction) * fraction * (1.0 - fraction) / 6.0
    return first, second, third, fourth


def advect_species(species_field, offsets, weights):
    columns = lax.broadcasted_iota(jnp.int32, offsets.shape, 1)
    departure = (columns - offsets).astype(jnp.int32)
    stencil = []
    for offset_tap in range(4):
        position = ((departure - 1 + offset_tap) % NLON).astype(jnp.int32)
        stencil.append(jnp.take_along_axis(species_field, position, axis=1))
    cubic = weights[0] * stencil[0] + weights[1] * stencil[1]
    cubic = cubic + weights[2] * stencil[2] + weights[3] * stencil[3]
    lower_bound = jnp.minimum(stencil[1], stencil[2])
    upper_bound = jnp.maximum(stencil[1], stencil[2])
    return jnp.clip(cubic, lower_bound, upper_bound)


def reference(tracer, offsets, frac, air_before, air_after, growth):
    weights = tuple(item[:, None, :] for item in cubic_weights(frac))
    before_mass = jnp.sum(tracer * air_before[None], axis=(1, 2, 3))
    limited = lax.map(lambda field: advect_species(field, offsets, weights), tracer)
    after_mass = jnp.sum(limited * air_after[None], axis=(1, 2, 3))
    factor = before_mass * (1.0 + growth) / after_mass
    return limited * factor[:, None, None, None]
```

```python
import functools

import jax
import jax.numpy as jnp
from jax import lax
from jax.experimental import pallas as pl
from jax.experimental.pallas import tpu as pltpu
from jax.sharding import PartitionSpec as P

OFFMAX = 12
LANES = 128
ROWS = 8
LOW = OFFMAX + 1
HIGH = OFFMAX + 2
MESH = pl.DeviceIdType.MESH


def cubic_weights(fraction):
    first = -fraction * (1.0 - fraction) * (2.0 - fraction) / 6.0
    second = (1.0 + fraction) * (1.0 - fraction) * (2.0 - fraction) / 2.0
    third = (1.0 + fraction) * fraction * (2.0 - fraction) / 2.0
    fourth = -(1.0 + fraction) * fraction * (1.0 - fraction) / 6.0
    return (first, second, third, fourth)


def pick(bits, items):
    for bit in bits:
        merged = [jnp.where(bit, items[j + 1], items[j]) for j in range(0, len(items) - 1, 2)]
        if len(items) % 2:
            merged.append(items[-1])
        items = merged
    return items[0]


def kernel(
    dims,
    tracer,
    offsets,
    air_before,
    air_after,
    frac,
    growth,
    out,
    t_in,
    off_in,
    ab_in,
    aa_in,
    t_col,
    k_col,
    ab_col,
    aa_col,
    g_col,
    g_out,
    g_halo,
    f_col,
    weight,
    acc,
    factor,
    row_own,
    row_pair,
    rows_near,
    row_far_out,
    row_far,
    row_side,
    row_other,
    in_sem,
    small_in_sem,
    out_sem,
    edge_send,
    edge_recv,
    g_send,
    g_recv,
    bulk_send,
    bulk_recv,
    know,
    pair_send,
    pair_recv,
    near_send,
    near_recv,
    far_send,
    far_recv,
):
    S, L, W, n = dims
    blocks = W // ROWS
    reach = n // 8
    me = lax.axis_index("lon")
    core = lax.rem(me, 2)
    left, right = lax.rem(me + n - 1, n), lax.rem(me + 1, n)
    partner = me + 1 - 2 * core

    def away(distance):
        return lax.rem(me + distance + n, n)

    barrier = pltpu.get_barrier_semaphore()
    for to in (left, right):
        pl.semaphore_signal(barrier, inc=1, device_id={"lon": to}, device_id_type=MESH)

    load_off = pltpu.make_async_copy(offsets, off_in, small_in_sem.at[0])
    load_aa = pltpu.make_async_copy(air_after, aa_in, small_in_sem.at[1])
    load_ab = pltpu.make_async_copy(air_before, ab_in, small_in_sem.at[2])
    load_off.start()
    load_aa.start()
    load_ab.start()
    for s in range(S):
        pltpu.make_async_copy(tracer.at[s], t_in.at[s], in_sem.at[s]).start()

    def remote(src, dst, send, recv, to):
        return pltpu.make_async_remote_copy(
            src_ref=src, dst_ref=dst, send_sem=send, recv_sem=recv, device_id={"lon": to}, device_id_type=MESH
        )

    edge_up = remote(
        t_col.at[:, :, pl.ds(LOW + W - 1, 1)], t_col.at[:, :, pl.ds(LOW - 1, 1)], edge_send.at[0], edge_recv.at[0], right
    )
    edge_down = remote(
        t_col.at[:, :, pl.ds(LOW, 2)], t_col.at[:, :, pl.ds(LOW + W, 2)], edge_send.at[1], edge_recv.at[1], left
    )
    g_down = remote(g_out.at[0], g_halo.at[1], g_send.at[0], g_recv.at[0], left)
    g_up = remote(g_out.at[1], g_halo.at[0], g_send.at[1], g_recv.at[1], right)

    def bulk_up(s):
        return remote(
            t_col.at[s, :, pl.ds(W, OFFMAX)], t_col.at[s, :, pl.ds(0, OFFMAX)], bulk_send.at[0, s], bulk_recv.at[0, s], right
        )

    def bulk_down(s):
        return remote(
            t_col.at[s, :, pl.ds(LOW + 2, OFFMAX)],
            t_col.at[s, :, pl.ds(LOW + W + 2, OFFMAX)],
            bulk_send.at[1, s],
            bulk_recv.at[1, s],
            left,
        )

    rounds = know.shape[0]

    def tell(r):
        if r >= rounds:
            return
        for side, distance in ((0, 2**r), (1, -(2**r))):
            pl.semaphore_signal(know.at[r, side], inc=1, device_id={"lon": away(distance)}, device_id_type=MESH)

    def hear(r):
        if r >= rounds:
            return
        for side in range(2):
            pl.semaphore_wait(know.at[r, side], 1)

    load_off.wait()
    load_aa.wait()

    def relay_small(x, _):
        lev, blk = x // blocks, lax.rem(x, blocks)
        for l in range(ROWS):
            k_col[lev, blk * ROWS + l] = OFFMAX - off_in[lev, blk, pl.ds(l, ROWS, stride=ROWS), :]
            aa_col[lev, blk * ROWS + l] = aa_in[lev, blk, pl.ds(l, ROWS, stride=ROWS), :]
        return 0

    lax.fori_loop(0, L * blocks, relay_small, 0)

    def weight_of(lev, b):
        total = None
        for i in range(max(0, b - OFFMAX), min(W - 1, b + OFFMAX) + 1):
            term = jnp.where(k_col[lev, i] == OFFMAX - i + b, aa_col[lev, i], 0.0)
            total = term if total is None else total + term
        return total

    def g_sides(lev, _):
        for j in range(OFFMAX):
            g_out[0, lev, j] = weight_of(lev, j - OFFMAX)
            g_out[1, lev, j] = weight_of(lev, W + j)
        return 0

    lax.fori_loop(0, L, g_sides, 0)

    for lev in range(L):
        for j in range(ROWS):
            weight[0, lev, j : j + 1, :] = frac[lev : lev + 1, j * LANES : (j + 1) * LANES]
        for tap, w in enumerate(cubic_weights(weight[0, lev])):
            weight[tap, lev] = w

    pl.semaphore_wait(barrier, 2)
    g_down.start()
    g_up.start()
    tell(0)

    load_ab.wait()

    def relay_before(x, _):
        lev, blk = x // blocks, lax.rem(x, blocks)
        for l in range(ROWS):
            ab_col[lev, blk * ROWS + l] = ab_in[lev, blk, pl.ds(l, ROWS, stride=ROWS), :]
        return 0

    lax.fori_loop(0, L * blocks, relay_before, 0)

    def relay_species(s, _):
        pltpu.make_async_copy(tracer.at[s], t_in.at[s], in_sem.at[s]).wait()

        def relay(x, totals):
            lev, blk = x // blocks, lax.rem(x, blocks)
            totals = list(totals)
            for l in range(ROWS):
                value = t_in[s, lev, blk, pl.ds(l, ROWS, stride=ROWS), :]
                t_col[s, lev, LOW + blk * ROWS + l] = value
                totals[l % 4] = totals[l % 4] + value * ab_col[lev, blk * ROWS + l]
            return tuple(totals)

        zero = jnp.zeros((ROWS, LANES), jnp.float32)
        totals = lax.fori_loop(0, L * blocks, relay, (zero,) * 4)
        acc[s] = (totals[0] + totals[1]) + (totals[2] + totals[3])
        return 0

    lax.fori_loop(0, S, relay_species, 0)
    hear(0)
    tell(1)
    edge_up.start()
    edge_down.start()

    def send_bulk(s, _):
        bulk_up(s).start()
        bulk_down(s).start()
        return 0

    lax.fori_loop(0, S, send_bulk, 0)

    def g_inside(lev, _):
        for b in range(W):
            g_col[lev, b] = weight_of(lev, b)
        return 0

    lax.fori_loop(0, L, g_inside, 0)
    hear(1)
    tell(2)

    def departures(s, lev, first, count):
        w = [weight[tap, lev] for tap in range(4)]
        t = [t_col[s, lev, LOW + first - 1 + j] for j in range(count + 3)]
        for j in range(count):
            cubic = w[0] * t[j] + w[1] * t[j + 1]
            cubic = cubic + w[2] * t[j + 2] + w[3] * t[j + 3]
            low, high = jnp.minimum(t[j + 1], t[j + 2]), jnp.maximum(t[j + 1], t[j + 2])
            f_col[s, lev, OFFMAX + first + j] = jnp.minimum(jnp.maximum(cubic, low), high)

    def inside(x, _):
        s, lev = x // L, lax.rem(x, L)
        for first in range(1, W - 2, ROWS):
            departures(s, lev, first, min(ROWS, W - 2 - first))
        return 0

    lax.fori_loop(0, S * L, inside, 0)
    hear(2)
    tell(3)

    edge_up.wait_recv()
    edge_down.wait_recv()
    g_down.wait_recv()
    g_up.wait_recv()

    def g_total(lev, _):
        for j in range(OFFMAX):
            g_col[lev, j] = g_col[lev, j] + g_halo[0, lev, j]
            g_col[lev, W - OFFMAX + j] = g_col[lev, W - OFFMAX + j] + g_halo[1, lev, j]
        return 0

    lax.fori_loop(0, L, g_total, 0)

    def after_mass(s, _):
        def level(lev, totals):
            totals = list(totals)
            departures(s, lev, 0, 1)
            departures(s, lev, W - 2, 2)
            for b in range(W):
                totals[b % 4] = totals[b % 4] + f_col[s, lev, OFFMAX + b] * g_col[lev, b]
            return tuple(totals)

        zero = jnp.zeros((ROWS, LANES), jnp.float32)
        totals = lax.fori_loop(0, L, level, (zero,) * 4)
        acc[S + s] = (totals[0] + totals[1]) + (totals[2] + totals[3])
        return 0

    lax.fori_loop(0, S, after_mass, 0)

    sums = jnp.sum(jnp.sum(acc[...], axis=1), axis=1, keepdims=True)
    at_row = lax.broadcasted_iota(jnp.int32, (2 * S, LANES), 0)
    at_lane = lax.broadcasted_iota(jnp.int32, (2 * S, LANES), 1)
    row_own[...] = jnp.sum(jnp.where(at_row == at_lane, sums, 0.0), axis=0, keepdims=True)

    pair = remote(row_own, row_pair, pair_send.at[0], pair_recv.at[0], partner)
    pair.start()
    pair.wait_recv()
    row_own_chip = row_own[...] + row_pair[...]
    row_side[...] = row_own_chip
    for r in range(3, rounds):
        hear(r)
        if r + 1 < rounds:
            tell(r + 1)

    way = 2 * (1 - 2 * core)
    near = [
        remote(row_side, rows_near.at[d], near_send.at[d], near_recv.at[d], away(way * (d + 1))) for d in range(reach)
    ]
    for copy in near:
        copy.start()

    def cells(s, _):
        bulk_up(s).wait_recv()
        bulk_down(s).wait_recv()

        def halo(lev, _):
            for first in (-OFFMAX, -OFFMAX + 6, W, W + 6):
                departures(s, lev, first, 6)
            return 0

        lax.fori_loop(0, L, halo, 0)

        def gather(x, _):
            lev, blk = x // blocks, lax.rem(x, blocks)
            base = blk * ROWS
            f = [f_col[s, lev, base + j] for j in range(ROWS + 2 * OFFMAX)]
            for l in range(ROWS):
                k = k_col[lev, base + l]
                bits = [(k & (1 << bit)) != 0 for bit in range(5)]
                t_in[s, lev, blk, pl.ds(l, ROWS, stride=ROWS), :] = pick(bits, f[l : l + 2 * OFFMAX + 1])
            return 0

        lax.fori_loop(0, L * blocks, gather, 0)
        return 0

    lax.fori_loop(0, S // 2, cells, 0)

    for copy in near:
        copy.wait_recv()
    sided = jnp.sum(rows_near[...], axis=0)
    last = jnp.where(core == 0, 1.0, 0.0)
    row_far_out[...] = jnp.sum(rows_near[pl.ds(0, reach - 1)], axis=0) + last * rows_near[reach - 1]
    far = remote(row_far_out, row_far, far_send.at[0], far_recv.at[0], away(way * reach))
    far.start()

    lax.fori_loop(S // 2, S - 1, cells, 0)

    far.wait_recv()
    row_pair_side = sided + row_far[...]
    row_far_out_2 = row_other.at[0]
    row_far_out_2[...] = row_pair_side
    swap = remote(row_other.at[0], row_other.at[1], pair_send.at[1], pair_recv.at[1], partner)
    swap.start()

    lax.fori_loop(S - 1, S, cells, 0)

    swap.wait_recv()
    total = row_side[...] + (row_other[0] + row_other[1])
    spread = jnp.broadcast_to(total, (S, LANES))
    at_row = lax.broadcasted_iota(jnp.int32, (S, LANES), 0)
    at_lane = lax.broadcasted_iota(jnp.int32, (S, LANES), 1)
    before = jnp.sum(jnp.where(at_lane == at_row, spread, 0.0), axis=1, keepdims=True)
    after = jnp.sum(jnp.where(at_lane == at_row + S, spread, 0.0), axis=1, keepdims=True)
    gain = jnp.zeros((S, LANES), jnp.float32)
    for s in range(S):
        gain = jnp.where(at_row == s, 1.0 + growth[s], gain)
    ratio = before * gain / after
    for s in range(S):
        factor[s] = jnp.broadcast_to(ratio[s : s + 1, :], (ROWS, LANES))

    def scale(s, _):
        def part(x, _):
            lev, blk = x // blocks, lax.rem(x, blocks)
            for l in range(ROWS):
                rows = pl.ds(l * ROWS, ROWS)
                t_in[s, lev, blk, rows, :] = t_in[s, lev, blk, rows, :] * factor[s]
            return 0

        lax.fori_loop(0, L * blocks, part, 0)
        pltpu.make_async_copy(t_in.at[s], out.at[s], out_sem.at[s]).start()
        return 0

    lax.fori_loop(0, S, scale, 0)

    edge_up.wait_send()
    edge_down.wait_send()
    g_down.wait_send()
    g_up.wait_send()
    pair.wait_send()
    swap.wait_send()
    far.wait_send()
    for copy in near:
        copy.wait_send()

    def finish(s, _):
        bulk_up(s).wait_send()
        bulk_down(s).wait_send()
        pltpu.make_async_copy(t_in.at[s], out.at[s], out_sem.at[s]).wait()
        return 0

    lax.fori_loop(0, S, finish, 0)


def to_tiles(a):
    *lead, cols, lats = a.shape
    k = len(lead)
    a = a.reshape(*lead, cols // ROWS, ROWS, lats // LANES, LANES)
    a = a.transpose(*range(k), k, k + 2, k + 1, k + 3)
    return a.reshape(*lead, cols // ROWS, lats // LANES * ROWS, LANES)


def from_tiles(a, cols, lats):
    *lead, _, _, _ = a.shape
    k = len(lead)
    a = a.reshape(*lead, cols // ROWS, lats // LANES, ROWS, LANES)
    a = a.transpose(*range(k), k, k + 2, k + 1, k + 3)
    return a.reshape(*lead, cols, lats)


def on_device(n, tracer, offsets, frac, air_before, air_after, growth):
    S, L, W, lats = tracer.shape
    tiles = to_tiles(tracer)
    f32, vmem = jnp.float32, pltpu.VMEM
    column = (ROWS, LANES)
    blocks = W // ROWS
    dma = pltpu.SemaphoreType.DMA
    reach = n // 8
    rounds = reach.bit_length()
    small = (L, blocks, ROWS * ROWS, LANES)
    result = pl.pallas_call(
        functools.partial(kernel, (S, L, W, n)),
        out_shape=jax.ShapeDtypeStruct(tiles.shape, f32),
        in_specs=[pl.BlockSpec(memory_space=pl.ANY)] * 4
        + [pl.BlockSpec(memory_space=pltpu.VMEM), pl.BlockSpec(memory_space=pltpu.SMEM)],
        out_specs=pl.BlockSpec(memory_space=pl.ANY),
        scratch_shapes=[
            vmem(tiles.shape, f32),
            vmem(small, jnp.int32),
            vmem(small, f32),
            vmem(small, f32),
            vmem((S, L, LOW + W + HIGH, *column), f32),
            vmem((L, W, *column), jnp.int32),
            vmem((L, W, *column), f32),
            vmem((L, W, *column), f32),
            vmem((L, W, *column), f32),
            vmem((2, L, OFFMAX, *column), f32),
            vmem((2, L, OFFMAX, *column), f32),
            vmem((S, L, W + 2 * OFFMAX, *column), f32),
            vmem((4, L, *column), f32),
            vmem((2 * S, *column), f32),
            vmem((S, *column), f32),
            vmem((1, LANES), f32),
            vmem((1, LANES), f32),
            vmem((reach, 1, LANES), f32),
            vmem((1, LANES), f32),
            vmem((1, LANES), f32),
            vmem((1, LANES), f32),
            vmem((2, 1, LANES), f32),
            dma((S,)),
            dma((3,)),
            dma((S,)),
            dma((2,)),
            dma((2,)),
            dma((2,)),
            dma((2,)),
            dma((2, S)),
            dma((2, S)),
            pltpu.SemaphoreType.REGULAR((rounds, 2)),
            dma((2,)),
            dma((2,)),
            dma((reach,)),
            dma((reach,)),
            dma((1,)),
            dma((1,)),
        ],
        compiler_params=pltpu.CompilerParams(collective_id=0, has_side_effects=True),
    )(tiles, to_tiles(offsets), to_tiles(air_before), to_tiles(air_after), frac, growth)
    return from_tiles(result, W, lats)


def solution(mesh):
    placed = (
        P("scen", None, "lon", None),
        P(None, "lon", None),
        P(),
        P(None, "lon", None),
        P(None, "lon", None),
        P("scen"),
    )
    return jax.shard_map(
        functools.partial(on_device, mesh.shape["lon"]),
        mesh=mesh,
        in_specs=placed,
        out_specs=P("scen", None, "lon", None),
        check_vma=False,
    )
```

```python
import functools

import jax
import jax.numpy as jnp
from jax import lax
from jax.experimental import pallas as pl
from jax.experimental.pallas import tpu as pltpu
from jax.sharding import PartitionSpec as P

OFFMAX = 12
LANES = 128
ROWS = 8
LOW = OFFMAX + 1
HIGH = OFFMAX + 2
MESH = pl.DeviceIdType.MESH


def cubic_weights(fraction):
    first = -fraction * (1.0 - fraction) * (2.0 - fraction) / 6.0
    second = (1.0 + fraction) * (1.0 - fraction) * (2.0 - fraction) / 2.0
    third = (1.0 + fraction) * fraction * (2.0 - fraction) / 2.0
    fourth = -(1.0 + fraction) * fraction * (1.0 - fraction) / 6.0
    return (first, second, third, fourth)


def pick(bits, items):
    for bit in bits:
        merged = [jnp.where(bit, items[j + 1], items[j]) for j in range(0, len(items) - 1, 2)]
        if len(items) % 2:
            merged.append(items[-1])
        items = merged
    return items[0]


def kernel(
    dims,
    tracer,
    offsets,
    air_before,
    air_after,
    frac,
    growth,
    out,
    t_in,
    frac_in,
    growth_in,
    off_in,
    ab_in,
    aa_in,
    t_col,
    k_col,
    ab_col,
    aa_col,
    g_col,
    g_out,
    g_halo,
    f_col,
    weight,
    acc,
    factor,
    row_own,
    row_pair,
    row_chip,
    rows_near,
    row_far_out,
    rows_far,
    edge_in_sem,
    in_sem,
    small_in_sem,
    edge_send,
    edge_recv,
    g_send,
    g_recv,
    bulk_send,
    bulk_recv,
    know,
    pair_send,
    pair_recv,
    near_send,
    near_recv,
    far_send,
    far_recv,
):
    S, L, W, n = dims
    blocks = W // ROWS
    reach = n // 8
    me = lax.axis_index("lon")
    core = lax.rem(me, 2)
    left, right = lax.rem(me + n - 1, n), lax.rem(me + 1, n)
    partner = me + 1 - 2 * core

    def away(distance):
        return lax.rem(me + distance + n, n)

    barrier = pltpu.get_barrier_semaphore()
    for to in (left, right):
        pl.semaphore_signal(barrier, inc=1, device_id={"lon": to}, device_id_type=MESH)

    load_edges = [
        pltpu.make_async_copy(tracer.at[:, :, blk], t_in.at[:, :, blk], edge_in_sem.at[i])
        for i, blk in enumerate((0, blocks - 1))
    ]
    load_off = pltpu.make_async_copy(offsets, off_in, small_in_sem.at[0])
    load_aa = pltpu.make_async_copy(air_after, aa_in, small_in_sem.at[1])
    load_ab = pltpu.make_async_copy(air_before, ab_in, small_in_sem.at[2])
    load_frac = pltpu.make_async_copy(frac, frac_in, small_in_sem.at[3])
    load_growth = pltpu.make_async_copy(growth, growth_in, small_in_sem.at[4])

    def load_inner(s):
        inner = pl.ds(1, blocks - 2)
        return pltpu.make_async_copy(tracer.at[s, :, inner], t_in.at[s, :, inner], in_sem.at[s])

    for copy in (*load_edges, load_off, load_aa, load_frac, load_ab, load_growth):
        copy.start()
    for s in range(S):
        load_inner(s).start()

    def remote(src, dst, send, recv, to):
        return pltpu.make_async_remote_copy(
            src_ref=src, dst_ref=dst, send_sem=send, recv_sem=recv, device_id={"lon": to}, device_id_type=MESH
        )

    edge_up = remote(
        t_col.at[:, :, pl.ds(LOW + W - 1, 1)], t_col.at[:, :, pl.ds(LOW - 1, 1)], edge_send.at[0], edge_recv.at[0], right
    )
    edge_down = remote(
        t_col.at[:, :, pl.ds(LOW, 2)], t_col.at[:, :, pl.ds(LOW + W, 2)], edge_send.at[1], edge_recv.at[1], left
    )
    g_down = remote(g_out.at[0], g_halo.at[1], g_send.at[0], g_recv.at[0], left)
    g_up = remote(g_out.at[1], g_halo.at[0], g_send.at[1], g_recv.at[1], right)

    def bulk_up(s):
        return remote(
            t_col.at[s, :, pl.ds(W, OFFMAX)], t_col.at[s, :, pl.ds(0, OFFMAX)], bulk_send.at[0, s], bulk_recv.at[0, s], right
        )

    def bulk_down(s):
        return remote(
            t_col.at[s, :, pl.ds(LOW + 2, OFFMAX)],
            t_col.at[s, :, pl.ds(LOW + W + 2, OFFMAX)],
            bulk_send.at[1, s],
            bulk_recv.at[1, s],
            left,
        )

    rounds = know.shape[0]

    steps = [2**r for r in range(rounds - 1)] + [1]

    def tell(r):
        if r >= rounds:
            return
        for side, distance in ((0, steps[r]), (1, -steps[r])):
            pl.semaphore_signal(know.at[r, side], inc=1, device_id={"lon": away(distance)}, device_id_type=MESH)

    def hear(r):
        if r >= rounds:
            return
        for side in range(2):
            pl.semaphore_wait(know.at[r, side], 1)

    for copy in load_edges:
        copy.wait()

    def relay_edges(s, _):
        for lev in range(L):
            for blk, l in ((0, 0), (0, 1), (blocks - 1, ROWS - 1)):
                t_col[s, lev, LOW + blk * ROWS + l] = t_in[s, lev, blk, pl.ds(l, ROWS, stride=ROWS), :]
        return 0

    lax.fori_loop(0, S, relay_edges, 0)
    load_off.wait()
    load_aa.wait()
    pl.semaphore_wait(barrier, 2)
    edge_down.start()
    edge_up.start()
    tell(0)

    def relay_small(x, _):
        lev, blk = x // blocks, lax.rem(x, blocks)
        for l in range(ROWS):
            k_col[lev, blk * ROWS + l] = OFFMAX - off_in[lev, blk, pl.ds(l, ROWS, stride=ROWS), :]
            aa_col[lev, blk * ROWS + l] = aa_in[lev, blk, pl.ds(l, ROWS, stride=ROWS), :]
        return 0

    lax.fori_loop(0, L * blocks, relay_small, 0)

    def weight_of(lev, b):
        total = None
        for i in range(max(0, b - OFFMAX), min(W - 1, b + OFFMAX) + 1):
            term = jnp.where(k_col[lev, i] == OFFMAX - i + b, aa_col[lev, i], 0.0)
            total = term if total is None else total + term
        return total

    def g_sides(lev, _):
        for j in range(OFFMAX):
            g_out[0, lev, j] = weight_of(lev, j - OFFMAX)
            g_out[1, lev, j] = weight_of(lev, W + j)
        return 0

    lax.fori_loop(0, L, g_sides, 0)
    load_frac.wait()
    for lev in range(L):
        for j in range(ROWS):
            weight[0, lev, j : j + 1, :] = frac_in[lev : lev + 1, j * LANES : (j + 1) * LANES]
        for tap, w in enumerate(cubic_weights(weight[0, lev])):
            weight[tap, lev] = w
    g_down.start()
    g_up.start()
    hear(0)
    tell(1)

    load_ab.wait()

    def relay_before(x, _):
        lev, blk = x // blocks, lax.rem(x, blocks)
        for l in range(ROWS):
            ab_col[lev, blk * ROWS + l] = ab_in[lev, blk, pl.ds(l, ROWS, stride=ROWS), :]
        return 0

    lax.fori_loop(0, L * blocks, relay_before, 0)

    zero = jnp.zeros((ROWS, LANES), jnp.float32)

    def relay_species(s, _):
        load_inner(s).wait()

        def relay(lev, totals):
            totals = list(totals)
            for i in range(W):
                blk, l = divmod(i, ROWS)
                if 2 <= i < W - 1:
                    value = t_in[s, lev, blk, pl.ds(l, ROWS, stride=ROWS), :]
                    t_col[s, lev, LOW + i] = value
                else:
                    value = t_col[s, lev, LOW + i]
                totals[i % 4] = totals[i % 4] + value * ab_col[lev, i]
            return tuple(totals)

        totals = lax.fori_loop(0, L, relay, (zero,) * 4)
        acc[s] = (totals[0] + totals[1]) + (totals[2] + totals[3])
        return 0

    lax.fori_loop(0, S, relay_species, 0)
    hear(1)
    tell(2)

    def send_bulk(s, _):
        bulk_up(s).start()
        bulk_down(s).start()
        return 0

    lax.fori_loop(0, S, send_bulk, 0)

    def g_inside(lev, _):
        for b in range(W):
            g_col[lev, b] = weight_of(lev, b)
        return 0

    lax.fori_loop(0, L, g_inside, 0)
    hear(2)
    tell(3)

    def departures(s, lev, first, count):
        w = [weight[tap, lev] for tap in range(4)]
        t = [t_col[s, lev, LOW + first - 1 + j] for j in range(count + 3)]
        values = []
        for j in range(count):
            cubic = w[0] * t[j] + w[1] * t[j + 1]
            cubic = cubic + w[2] * t[j + 2] + w[3] * t[j + 3]
            low, high = jnp.minimum(t[j + 1], t[j + 2]), jnp.maximum(t[j + 1], t[j + 2])
            values.append(jnp.minimum(jnp.maximum(cubic, low), high))
            f_col[s, lev, OFFMAX + first + j] = values[-1]
        return values

    def inside(s, _):
        def level(lev, totals):
            totals = list(totals)
            for first in range(1, W - 2, ROWS):
                for j, value in enumerate(departures(s, lev, first, min(ROWS, W - 2 - first))):
                    totals[j % 4] = totals[j % 4] + value * g_col[lev, first + j]
            return tuple(totals)

        totals = lax.fori_loop(0, L, level, (zero,) * 4)
        acc[S + s] = (totals[0] + totals[1]) + (totals[2] + totals[3])
        return 0

    lax.fori_loop(0, S, inside, 0)
    hear(3)
    tell(4)

    edge_up.wait_recv()
    edge_down.wait_recv()
    g_down.wait_recv()
    g_up.wait_recv()

    def outer_mass(lev, totals):
        g_low = [g_halo[0, lev, j] for j in range(OFFMAX)]
        g_high = [g_halo[1, lev, j] for j in range(OFFMAX)]
        sums = []
        for s in range(S):
            parts = [totals[s], zero]
            (first,) = departures(s, lev, 0, 1)
            last = departures(s, lev, W - 2, 2)
            parts[0] = parts[0] + first * g_col[lev, 0]
            parts[1] = parts[1] + last[0] * g_col[lev, W - 2]
            parts[1] = parts[1] + last[1] * g_col[lev, W - 1]
            for j in range(OFFMAX):
                low = first if j == 0 else f_col[s, lev, OFFMAX + j]
                at = W - OFFMAX + j
                high = last[at - W + 2] if at >= W - 2 else f_col[s, lev, OFFMAX + at]
                parts[0] = parts[0] + low * g_low[j]
                parts[1] = parts[1] + high * g_high[j]
            sums.append(parts[0] + parts[1])
        return tuple(sums)

    totals = lax.fori_loop(0, L, outer_mass, tuple(acc[S + s] for s in range(S)))
    for s in range(S):
        acc[S + s] = totals[s]

    sums = jnp.sum(jnp.sum(acc[...], axis=1), axis=1, keepdims=True)
    at_row = lax.broadcasted_iota(jnp.int32, (2 * S, LANES), 0)
    at_lane = lax.broadcasted_iota(jnp.int32, (2 * S, LANES), 1)
    row_own[...] = jnp.sum(jnp.where(at_row == at_lane, sums, 0.0), axis=0, keepdims=True)

    pair = remote(row_own, row_pair, pair_send.at[0], pair_recv.at[0], partner)
    pair.start()
    pair.wait_recv()
    row_chip[...] = row_own[...] + row_pair[...]
    for r in range(4, rounds):
        hear(r)
        tell(r + 1)

    way = 2 * (1 - 2 * core)

    def to_chip(d, at):
        return away(way * d - core + at)

    near = [
        remote(row_chip, rows_near.at[core, d], near_send.at[at, d], near_recv.at[core, d], to_chip(d + 1, at))
        for d in range(reach)
        for at in range(2)
    ]
    for copy in near:
        copy.start()

    def near_from(side, d):
        return remote(row_chip, rows_near.at[side, d], near_send.at[0, d], near_recv.at[side, d], partner)

    def cells(s, _):
        bulk_up(s).wait_recv()
        bulk_down(s).wait_recv()

        def halo(lev, _):
            for first in (-OFFMAX, -OFFMAX + 6, W, W + 6):
                departures(s, lev, first, 6)
            return 0

        lax.fori_loop(0, L, halo, 0)

        def gather(x, _):
            lev, blk = x // blocks, lax.rem(x, blocks)
            base = blk * ROWS
            f = [f_col[s, lev, base + j] for j in range(ROWS + 2 * OFFMAX)]
            for l in range(ROWS):
                k = k_col[lev, base + l]
                bits = [(k & (1 << bit)) != 0 for bit in range(5)]
                out[s, lev, blk, pl.ds(l, ROWS, stride=ROWS), :] = pick(bits, f[l : l + 2 * OFFMAX + 1])
            return 0

        lax.fori_loop(0, L * blocks, gather, 0)
        return 0

    early = S // 2 - 1
    lax.fori_loop(0, early, cells, 0)

    for side in range(2):
        for d in range(reach):
            near_from(side, d).wait_recv()
    mine = jnp.sum(rows_near[core, pl.ds(0, reach - 1)], axis=0)
    row_far_out[...] = mine + jnp.where(core == 0, 1.0, 0.0) * rows_near[core, reach - 1]
    far = [
        remote(row_far_out, rows_far.at[core], far_send.at[at], far_recv.at[core], to_chip(reach, at)) for at in range(2)
    ]
    for copy in far:
        copy.start()
    near_total = row_chip[...] + jnp.sum(rows_near[0], axis=0) + jnp.sum(rows_near[1], axis=0)

    lax.fori_loop(early, S, cells, 0)

    for side in range(2):
        remote(row_far_out, rows_far.at[side], far_send.at[0], far_recv.at[side], partner).wait_recv()
    load_growth.wait()
    total = near_total + (rows_far[0] + rows_far[1])
    spread = jnp.broadcast_to(total, (S, LANES))
    at_row = lax.broadcasted_iota(jnp.int32, (S, LANES), 0)
    at_lane = lax.broadcasted_iota(jnp.int32, (S, LANES), 1)
    before = jnp.sum(jnp.where(at_lane == at_row, spread, 0.0), axis=1, keepdims=True)
    after = jnp.sum(jnp.where(at_lane == at_row + S, spread, 0.0), axis=1, keepdims=True)
    gain = jnp.zeros((S, LANES), jnp.float32)
    for s in range(S):
        gain = jnp.where(at_row == s, 1.0 + growth_in[s], gain)
    ratio = before * gain / after
    for s in range(S):
        factor[s] = jnp.broadcast_to(ratio[s : s + 1, :], (ROWS, LANES))

    def scale(s, _):
        def part(x, _):
            lev, blk = x // blocks, lax.rem(x, blocks)
            for l in range(ROWS):
                rows = pl.ds(l * ROWS, ROWS)
                out[s, lev, blk, rows, :] = out[s, lev, blk, rows, :] * factor[s]
            return 0

        lax.fori_loop(0, L * blocks, part, 0)
        return 0

    lax.fori_loop(0, S, scale, 0)

    edge_up.wait_send()
    edge_down.wait_send()
    g_down.wait_send()
    g_up.wait_send()
    pair.wait_send()
    for copy in (*near, *far):
        copy.wait_send()

    def finish(s, _):
        bulk_up(s).wait_send()
        bulk_down(s).wait_send()
        return 0

    lax.fori_loop(0, S, finish, 0)


def to_tiles(a):
    *lead, cols, lats = a.shape
    k = len(lead)
    a = a.reshape(*lead, cols // ROWS, ROWS, lats // LANES, LANES)
    a = a.transpose(*range(k), k, k + 2, k + 1, k + 3)
    return a.reshape(*lead, cols // ROWS, lats // LANES * ROWS, LANES)


def from_tiles(a, cols, lats):
    *lead, _, _, _ = a.shape
    k = len(lead)
    a = a.reshape(*lead, cols // ROWS, lats // LANES, ROWS, LANES)
    a = a.transpose(*range(k), k, k + 2, k + 1, k + 3)
    return a.reshape(*lead, cols, lats)


def in_hbm(a):
    return pltpu.with_memory_space_constraint(a, pltpu.HBM)


def on_device(n, tracer, offsets, frac, air_before, air_after, growth):
    S, L, W, lats = tracer.shape
    tiles = to_tiles(tracer)
    f32, vmem = jnp.float32, pltpu.VMEM
    column = (ROWS, LANES)
    blocks = W // ROWS
    dma = pltpu.SemaphoreType.DMA
    reach = n // 8
    rounds = reach.bit_length() + 1
    small = (L, blocks, ROWS * ROWS, LANES)
    result = pl.pallas_call(
        functools.partial(kernel, (S, L, W, n)),
        out_shape=pltpu.VMEM(tiles.shape, f32),
        in_specs=[pl.BlockSpec(memory_space=pltpu.HBM)] * 6,

        out_specs=pl.BlockSpec(memory_space=pltpu.VMEM),
        scratch_shapes=[
            vmem(tiles.shape, f32),
            vmem(frac.shape, f32),
            pltpu.SMEM(growth.shape, f32),
            vmem(small, jnp.int32),
            vmem(small, f32),
            vmem(small, f32),
            vmem((S, L, LOW + W + HIGH, *column), f32),
            vmem((L, W, *column), jnp.int32),
            vmem((L, W, *column), f32),
            vmem((L, W, *column), f32),
            vmem((L, W, *column), f32),
            vmem((2, L, OFFMAX, *column), f32),
            vmem((2, L, OFFMAX, *column), f32),
            vmem((S, L, W + 2 * OFFMAX, *column), f32),
            vmem((4, L, *column), f32),
            vmem((2 * S, *column), f32),
            vmem((S, *column), f32),
            vmem((1, LANES), f32),
            vmem((1, LANES), f32),
            vmem((1, LANES), f32),
            vmem((2, reach, 1, LANES), f32),
            vmem((1, LANES), f32),
            vmem((2, 1, LANES), f32),
            dma((2,)),
            dma((S,)),
            dma((5,)),
            dma((2,)),
            dma((2,)),
            dma((2,)),
            dma((2,)),
            dma((2, S)),
            dma((2, S)),
            pltpu.SemaphoreType.REGULAR((rounds, 2)),
            dma((1,)),
            dma((1,)),
            dma((2, reach)),
            dma((2, reach)),
            dma((2,)),
            dma((2,)),
        ],
        compiler_params=pltpu.CompilerParams(collective_id=0, has_side_effects=True, vmem_limit_bytes=44 * 2**20),
    )(*map(in_hbm, (tiles, to_tiles(offsets), to_tiles(air_before), to_tiles(air_after), frac, growth)))
    return from_tiles(result, W, lats)


def solution(mesh):
    placed = (
        P("scen", None, "lon", None),
        P(None, "lon", None),
        P(),
        P(None, "lon", None),
        P(None, "lon", None),
        P("scen"),
    )
    return jax.shard_map(
        functools.partial(on_device, mesh.shape["lon"]),
        mesh=mesh,
        in_specs=placed,
        out_specs=P("scen", None, "lon", None),
        check_vma=False,
    )
```

```python
import functools

import jax
import jax.numpy as jnp
from jax import lax
from jax.experimental import pallas as pl
from jax.experimental.pallas import tpu as pltpu
from jax.sharding import PartitionSpec as P

OFFMAX = 12
LANES = 128
ROWS = 8
LOW = OFFMAX + 1
HIGH = OFFMAX + 2
NEAR = 5
MESH = pl.DeviceIdType.MESH


def know_steps(known, wanted):
    steps = []
    while known < wanted:
        steps.append(min(known, wanted - known))
        known += steps[-1]
    return steps


def cubic_weights(fraction):
    first = -fraction * (1.0 - fraction) * (2.0 - fraction) / 6.0
    second = (1.0 + fraction) * (1.0 - fraction) * (2.0 - fraction) / 2.0
    third = (1.0 + fraction) * fraction * (2.0 - fraction) / 2.0
    fourth = -(1.0 + fraction) * fraction * (1.0 - fraction) / 6.0
    return (first, second, third, fourth)


def pick(bits, items):
    for bit in bits:
        merged = [jnp.where(bit, items[j + 1], items[j]) for j in range(0, len(items) - 1, 2)]
        if len(items) % 2:
            merged.append(items[-1])
        items = merged
    return items[0]


def kernel(
    dims,
    tracer,
    offsets,
    air_before,
    air_after,
    frac,
    growth,
    out,
    factor,
    t_in,
    frac_in,
    growth_in,
    off_in,
    ab_in,
    aa_in,
    t_col,
    k_col,
    ab_col,
    aa_col,
    g_col,
    g_out,
    g_halo,
    f_col,
    weight,
    acc,
    row_own,
    row_pair,
    row_chip,
    rows_near,
    row_far_out,
    rows_far,
    edge_in_sem,
    in_sem,
    small_in_sem,
    edge_send,
    edge_recv,
    g_send,
    g_recv,
    bulk_send,
    bulk_recv,
    know,
    pair_send,
    pair_recv,
    near_send,
    near_recv,
    far_send,
    far_recv,
):
    S, L, W, n = dims
    blocks = W // ROWS
    reach = n // 8
    me = lax.axis_index("lon")
    core = lax.rem(me, 2)
    left, right = lax.rem(me + n - 1, n), lax.rem(me + 1, n)
    partner = me + 1 - 2 * core

    def away(distance):
        return lax.rem(me + distance + n, n)

    barrier = pltpu.get_barrier_semaphore()
    close_by = min(NEAR, n // 2 - 1)
    for distance in range(1, close_by + 1):
        for to in (away(distance), away(-distance)):
            pl.semaphore_signal(barrier, inc=1, device_id={"lon": to}, device_id_type=MESH)

    load_edges = [
        pltpu.make_async_copy(tracer.at[:, :, blk], t_in.at[:, :, blk], edge_in_sem.at[i])
        for i, blk in enumerate((0, blocks - 1))
    ]
    load_off = pltpu.make_async_copy(offsets, off_in, small_in_sem.at[0])
    load_aa = pltpu.make_async_copy(air_after, aa_in, small_in_sem.at[1])
    load_ab = pltpu.make_async_copy(air_before, ab_in, small_in_sem.at[2])
    load_frac = pltpu.make_async_copy(frac, frac_in, small_in_sem.at[3])
    load_growth = pltpu.make_async_copy(growth, growth_in, small_in_sem.at[4])

    def load_inner(s):
        inner = pl.ds(1, blocks - 2)
        return pltpu.make_async_copy(tracer.at[s, :, inner], t_in.at[s, :, inner], in_sem.at[s])

    for copy in (*load_edges, load_off, load_aa, load_frac, load_ab, load_growth):
        copy.start()
    for s in range(S):
        load_inner(s).start()

    def remote(src, dst, send, recv, to):
        return pltpu.make_async_remote_copy(
            src_ref=src, dst_ref=dst, send_sem=send, recv_sem=recv, device_id={"lon": to}, device_id_type=MESH
        )

    edge_up = remote(
        t_col.at[:, :, pl.ds(LOW + W - 1, 1)], t_col.at[:, :, pl.ds(LOW - 1, 1)], edge_send.at[0], edge_recv.at[0], right
    )
    edge_down = remote(
        t_col.at[:, :, pl.ds(LOW, 2)], t_col.at[:, :, pl.ds(LOW + W, 2)], edge_send.at[1], edge_recv.at[1], left
    )
    g_down = remote(g_out.at[0], g_halo.at[1], g_send.at[0], g_recv.at[0], left)
    g_up = remote(g_out.at[1], g_halo.at[0], g_send.at[1], g_recv.at[1], right)

    def bulk_up(s):
        return remote(
            t_col.at[s, :, pl.ds(W, OFFMAX)], t_col.at[s, :, pl.ds(0, OFFMAX)], bulk_send.at[0, s], bulk_recv.at[0, s], right
        )

    def bulk_down(s):
        return remote(
            t_col.at[s, :, pl.ds(LOW + 2, OFFMAX)],
            t_col.at[s, :, pl.ds(LOW + W + 2, OFFMAX)],
            bulk_send.at[1, s],
            bulk_recv.at[1, s],
            left,
        )

    steps = know_steps(close_by, 2 * reach + 1)
    rounds = len(steps)

    def tell(r):
        if r >= rounds:
            return
        for side, distance in ((0, steps[r]), (1, -steps[r])):
            pl.semaphore_signal(know.at[r, side], inc=1, device_id={"lon": away(distance)}, device_id_type=MESH)

    def hear(r):
        if r >= rounds:
            return
        for side in range(2):
            pl.semaphore_wait(know.at[r, side], 1)

    for copy in load_edges:
        copy.wait()

    def relay_edges(s, _):
        for lev in range(L):
            for blk, l in ((0, 0), (0, 1), (blocks - 1, ROWS - 1)):
                t_col[s, lev, LOW + blk * ROWS + l] = t_in[s, lev, blk, pl.ds(l, ROWS, stride=ROWS), :]
        return 0

    lax.fori_loop(0, S, relay_edges, 0)
    load_off.wait()
    load_aa.wait()
    pl.semaphore_wait(barrier, 2 * close_by)
    edge_down.start()
    edge_up.start()
    tell(0)

    def relay_small(x, _):
        lev, blk = x // blocks, lax.rem(x, blocks)
        for l in range(ROWS):
            k_col[lev, blk * ROWS + l] = OFFMAX - off_in[lev, blk, pl.ds(l, ROWS, stride=ROWS), :]
            aa_col[lev, blk * ROWS + l] = aa_in[lev, blk, pl.ds(l, ROWS, stride=ROWS), :]
        return 0

    lax.fori_loop(0, L * blocks, relay_small, 0)

    def weight_of(lev, b):
        total = None
        for i in range(max(0, b - OFFMAX), min(W - 1, b + OFFMAX) + 1):
            term = jnp.where(k_col[lev, i] == OFFMAX - i + b, aa_col[lev, i], 0.0)
            total = term if total is None else total + term
        return total

    def g_sides(lev, _):
        for j in range(OFFMAX):
            g_out[0, lev, j] = weight_of(lev, j - OFFMAX)
            g_out[1, lev, j] = weight_of(lev, W + j)
        return 0

    lax.fori_loop(0, L, g_sides, 0)
    load_frac.wait()
    for lev in range(L):
        for j in range(ROWS):
            weight[0, lev, j : j + 1, :] = frac_in[lev : lev + 1, j * LANES : (j + 1) * LANES]
        for tap, w in enumerate(cubic_weights(weight[0, lev])):
            weight[tap, lev] = w
    g_down.start()
    g_up.start()
    load_ab.wait()

    def relay_before(x, _):
        lev, blk = x // blocks, lax.rem(x, blocks)
        for l in range(ROWS):
            ab_col[lev, blk * ROWS + l] = ab_in[lev, blk, pl.ds(l, ROWS, stride=ROWS), :]
        return 0

    lax.fori_loop(0, L * blocks, relay_before, 0)

    zero = jnp.zeros((ROWS, LANES), jnp.float32)

    def relay_species(s, _):
        load_inner(s).wait()

        def relay(lev, totals):
            totals = list(totals)
            for i in range(W):
                blk, l = divmod(i, ROWS)
                if 2 <= i < W - 1:
                    value = t_in[s, lev, blk, pl.ds(l, ROWS, stride=ROWS), :]
                    t_col[s, lev, LOW + i] = value
                else:
                    value = t_col[s, lev, LOW + i]
                totals[i % 4] = totals[i % 4] + value * ab_col[lev, i]
            return tuple(totals)

        totals = lax.fori_loop(0, L, relay, (zero,) * 4)
        acc[s] = (totals[0] + totals[1]) + (totals[2] + totals[3])
        return 0

    lax.fori_loop(0, S, relay_species, 0)
    def send_bulk(s, _):
        bulk_up(s).start()
        bulk_down(s).start()
        return 0

    lax.fori_loop(0, S, send_bulk, 0)

    def g_inside(lev, _):
        for b in range(W):
            g_col[lev, b] = weight_of(lev, b)
        return 0

    lax.fori_loop(0, L // 2, g_inside, 0)
    hear(0)
    tell(1)
    lax.fori_loop(L // 2, L, g_inside, 0)

    def departures(s, lev, first, count):
        w = [weight[tap, lev] for tap in range(4)]
        t = [t_col[s, lev, LOW + first - 1 + j] for j in range(count + 3)]
        values = []
        for j in range(count):
            cubic = w[0] * t[j] + w[1] * t[j + 1]
            cubic = cubic + w[2] * t[j + 2] + w[3] * t[j + 3]
            low, high = jnp.minimum(t[j + 1], t[j + 2]), jnp.maximum(t[j + 1], t[j + 2])
            values.append(jnp.minimum(jnp.maximum(cubic, low), high))
            f_col[s, lev, OFFMAX + first + j] = values[-1]
        return values

    def inside(s, _):
        def level(lev, totals):
            totals = list(totals)
            for first in range(1, W - 2, ROWS):
                for j, value in enumerate(departures(s, lev, first, min(ROWS, W - 2 - first))):
                    totals[j % 4] = totals[j % 4] + value * g_col[lev, first + j]
            return tuple(totals)

        totals = lax.fori_loop(0, L, level, (zero,) * 4)
        acc[S + s] = (totals[0] + totals[1]) + (totals[2] + totals[3])
        return 0

    lax.fori_loop(0, S, inside, 0)

    edge_up.wait_recv()
    edge_down.wait_recv()
    g_down.wait_recv()
    g_up.wait_recv()

    def outer_mass(lev, totals):
        g_low = [g_halo[0, lev, j] for j in range(OFFMAX)]
        g_high = [g_halo[1, lev, j] for j in range(OFFMAX)]
        sums = []
        for s in range(S):
            parts = [totals[s], zero]
            (first,) = departures(s, lev, 0, 1)
            last = departures(s, lev, W - 2, 2)
            parts[0] = parts[0] + first * g_col[lev, 0]
            parts[1] = parts[1] + last[0] * g_col[lev, W - 2]
            parts[1] = parts[1] + last[1] * g_col[lev, W - 1]
            for j in range(OFFMAX):
                low = first if j == 0 else f_col[s, lev, OFFMAX + j]
                at = W - OFFMAX + j
                high = last[at - W + 2] if at >= W - 2 else f_col[s, lev, OFFMAX + at]
                parts[0] = parts[0] + low * g_low[j]
                parts[1] = parts[1] + high * g_high[j]
            sums.append(parts[0] + parts[1])
        return tuple(sums)

    totals = lax.fori_loop(0, L, outer_mass, tuple(acc[S + s] for s in range(S)))
    for s in range(S):
        acc[S + s] = totals[s]

    sums = jnp.sum(jnp.sum(acc[...], axis=1), axis=1, keepdims=True)
    at_row = lax.broadcasted_iota(jnp.int32, (2 * S, LANES), 0)
    at_lane = lax.broadcasted_iota(jnp.int32, (2 * S, LANES), 1)
    row_own[...] = jnp.sum(jnp.where(at_row == at_lane, sums, 0.0), axis=0, keepdims=True)

    pair = remote(row_own, row_pair, pair_send.at[0], pair_recv.at[0], partner)
    pair.start()
    pair.wait_recv()
    row_chip[...] = row_own[...] + row_pair[...]
    for r in range(1, rounds):
        hear(r)
        tell(r + 1)

    way = 2 * (1 - 2 * core)

    def to_chip(d, at):
        return away(way * d - core + at)

    near = [
        remote(row_chip, rows_near.at[core, d], near_send.at[at, d], near_recv.at[core, d], to_chip(d + 1, at))
        for d in range(reach)
        for at in range(2)
    ]
    for copy in near:
        copy.start()

    def near_from(side, d):
        return remote(row_chip, rows_near.at[side, d], near_send.at[0, d], near_recv.at[side, d], partner)

    def cells(s, _):
        bulk_up(s).wait_recv()
        bulk_down(s).wait_recv()

        def halo(lev, _):
            for first in (-OFFMAX, -OFFMAX + 6, W, W + 6):
                departures(s, lev, first, 6)
            return 0

        lax.fori_loop(0, L, halo, 0)

        def gather(x, _):
            lev, blk = x // blocks, lax.rem(x, blocks)
            base = blk * ROWS
            f = [f_col[s, lev, base + j] for j in range(ROWS + 2 * OFFMAX)]
            for l in range(ROWS):
                k = k_col[lev, base + l]
                bits = [(k & (1 << bit)) != 0 for bit in range(5)]
                out[s, lev, blk, pl.ds(l, ROWS, stride=ROWS), :] = pick(bits, f[l : l + 2 * OFFMAX + 1])
            return 0

        lax.fori_loop(0, L * blocks, gather, 0)
        return 0

    early = S // 2 - 1
    lax.fori_loop(0, early, cells, 0)

    for side in range(2):
        for d in range(reach):
            near_from(side, d).wait_recv()
    mine = jnp.sum(rows_near[core, pl.ds(0, reach - 1)], axis=0)
    row_far_out[...] = mine + jnp.where(core == 0, 1.0, 0.0) * rows_near[core, reach - 1]
    far = [
        remote(row_far_out, rows_far.at[core], far_send.at[at], far_recv.at[core], to_chip(reach, at)) for at in range(2)
    ]
    for copy in far:
        copy.start()
    near_total = row_chip[...] + jnp.sum(rows_near[0], axis=0) + jnp.sum(rows_near[1], axis=0)

    lax.fori_loop(early, S, cells, 0)

    for side in range(2):
        remote(row_far_out, rows_far.at[side], far_send.at[0], far_recv.at[side], partner).wait_recv()
    load_growth.wait()
    total = near_total + (rows_far[0] + rows_far[1])
    spread = jnp.broadcast_to(total, (S, LANES))
    at_row = lax.broadcasted_iota(jnp.int32, (S, LANES), 0)
    at_lane = lax.broadcasted_iota(jnp.int32, (S, LANES), 1)
    before = jnp.sum(jnp.where(at_lane == at_row, spread, 0.0), axis=1, keepdims=True)
    after = jnp.sum(jnp.where(at_lane == at_row + S, spread, 0.0), axis=1, keepdims=True)
    gain = jnp.zeros((S, LANES), jnp.float32)
    for s in range(S):
        gain = jnp.where(at_row == s, 1.0 + growth_in[s], gain)
    ratio = before * gain / after
    for s in range(S):
        factor[s] = jnp.broadcast_to(ratio[s : s + 1, :], (ROWS, LANES))

    edge_up.wait_send()
    edge_down.wait_send()
    g_down.wait_send()
    g_up.wait_send()
    pair.wait_send()
    for copy in (*near, *far):
        copy.wait_send()

    def finish(s, _):
        bulk_up(s).wait_send()
        bulk_down(s).wait_send()
        return 0

    lax.fori_loop(0, S, finish, 0)


def scale_kernel(limited, factor, out, scaled, sem):
    S, L = limited.shape[:2]

    def put(s):
        return pltpu.make_async_copy(scaled.at[s], out.at[s], sem.at[s])

    def scale(s, _):
        gain = factor[s]

        def level(lev, _):
            for blk in range(limited.shape[2]):
                for row in range(0, limited.shape[3], ROWS):
                    scaled[s, lev, blk, pl.ds(row, ROWS), :] = limited[s, lev, blk, pl.ds(row, ROWS), :] * gain
            return 0

        lax.fori_loop(0, L, level, 0)
        put(s).start()
        return 0

    lax.fori_loop(0, S, scale, 0)
    for s in range(S):
        put(s).wait()


def to_tiles(a):
    *lead, cols, lats = a.shape
    k = len(lead)
    a = a.reshape(*lead, cols // ROWS, ROWS, lats // LANES, LANES)
    a = a.transpose(*range(k), k, k + 2, k + 1, k + 3)
    return a.reshape(*lead, cols // ROWS, lats // LANES * ROWS, LANES)


def from_tiles(a, cols, lats):
    *lead, _, _, _ = a.shape
    k = len(lead)
    a = a.reshape(*lead, cols // ROWS, lats // LANES, ROWS, LANES)
    a = a.transpose(*range(k), k, k + 2, k + 1, k + 3)
    return a.reshape(*lead, cols, lats)


def in_hbm(a):
    return pltpu.with_memory_space_constraint(a, pltpu.HBM)


def on_device(n, tracer, offsets, frac, air_before, air_after, growth):
    S, L, W, lats = tracer.shape
    tiles = to_tiles(tracer)
    f32, vmem = jnp.float32, pltpu.VMEM
    column = (ROWS, LANES)
    blocks = W // ROWS
    dma = pltpu.SemaphoreType.DMA
    reach = n // 8
    rounds = len(know_steps(min(NEAR, n // 2 - 1), 2 * reach + 1))
    small = (L, blocks, ROWS * ROWS, LANES)
    limited, factor = pl.pallas_call(
        functools.partial(kernel, (S, L, W, n)),
        out_shape=[pltpu.VMEM(tiles.shape, f32), pltpu.VMEM((S, *column), f32)],
        in_specs=[pl.BlockSpec(memory_space=pltpu.HBM)] * 6,

        out_specs=[pl.BlockSpec(memory_space=pltpu.VMEM)] * 2,
        scratch_shapes=[
            vmem(tiles.shape, f32),
            vmem(frac.shape, f32),
            pltpu.SMEM(growth.shape, f32),
            vmem(small, jnp.int32),
            vmem(small, f32),
            vmem(small, f32),
            vmem((S, L, LOW + W + HIGH, *column), f32),
            vmem((L, W, *column), jnp.int32),
            vmem((L, W, *column), f32),
            vmem((L, W, *column), f32),
            vmem((L, W, *column), f32),
            vmem((2, L, OFFMAX, *column), f32),
            vmem((2, L, OFFMAX, *column), f32),
            vmem((S, L, W + 2 * OFFMAX, *column), f32),
            vmem((4, L, *column), f32),
            vmem((2 * S, *column), f32),
            vmem((1, LANES), f32),
            vmem((1, LANES), f32),
            vmem((1, LANES), f32),
            vmem((2, reach, 1, LANES), f32),
            vmem((1, LANES), f32),
            vmem((2, 1, LANES), f32),
            dma((2,)),
            dma((S,)),
            dma((5,)),
            dma((2,)),
            dma((2,)),
            dma((2,)),
            dma((2,)),
            dma((2, S)),
            dma((2, S)),
            pltpu.SemaphoreType.REGULAR((rounds, 2)),
            dma((1,)),
            dma((1,)),
            dma((2, reach)),
            dma((2, reach)),
            dma((2,)),
            dma((2,)),
        ],
        compiler_params=pltpu.CompilerParams(collective_id=0, has_side_effects=True, vmem_limit_bytes=44 * 2**20),
    )(*map(in_hbm, (tiles, to_tiles(offsets), to_tiles(air_before), to_tiles(air_after), frac, growth)))
    result = pl.pallas_call(
        scale_kernel,
        out_shape=jax.ShapeDtypeStruct(tiles.shape, f32),
        in_specs=[pl.BlockSpec(memory_space=pltpu.VMEM)] * 2,
        out_specs=pl.BlockSpec(memory_space=pl.ANY),
        scratch_shapes=[vmem(tiles.shape, f32), dma((S,))],
        compiler_params=pltpu.CompilerParams(vmem_limit_bytes=24 * 2**20),
    )(limited, factor)
    return from_tiles(result, W, lats)


def solution(mesh):
    placed = (
        P("scen", None, "lon", None),
        P(None, "lon", None),
        P(),
        P(None, "lon", None),
        P(None, "lon", None),
        P("scen"),
    )
    return jax.shard_map(
        functools.partial(on_device, mesh.shape["lon"]),
        mesh=mesh,
        in_specs=placed,
        out_specs=P("scen", None, "lon", None),
        check_vma=False,
    )
```

```python
import functools

import jax
import jax.numpy as jnp
from jax import lax
from jax.experimental import pallas as pl
from jax.experimental.pallas import tpu as pltpu
from jax.sharding import PartitionSpec as P

OFFMAX = 12
LANES = 128
ROWS = 8
LOW = OFFMAX + 1
HIGH = OFFMAX + 2
MESH = pl.DeviceIdType.MESH


def know_steps(known, wanted):
    steps = []
    while known < wanted:
        steps.append(min(known, wanted - known))
        known += steps[-1]
    return steps


def cubic_weights(fraction):
    first = -fraction * (1.0 - fraction) * (2.0 - fraction) / 6.0
    second = (1.0 + fraction) * (1.0 - fraction) * (2.0 - fraction) / 2.0
    third = (1.0 + fraction) * fraction * (2.0 - fraction) / 2.0
    fourth = -(1.0 + fraction) * fraction * (1.0 - fraction) / 6.0
    return (first, second, third, fourth)


def pick(bits, items):
    for bit in bits:
        merged = [jnp.where(bit, items[j + 1], items[j]) for j in range(0, len(items) - 1, 2)]
        if len(items) % 2:
            merged.append(items[-1])
        items = merged
    return items[0]


def kernel(
    dims,
    tracer,
    offsets,
    air_before,
    air_after,
    frac,
    growth,
    out,
    factor,
    t_in,
    t_halo,
    frac_in,
    growth_in,
    off_in,
    ab_in,
    aa_in,
    t_col,
    k_col,
    ab_col,
    aa_col,
    g_col,
    g_out,
    g_halo,
    f_col,
    weight,
    acc,
    row_own,
    row_pair,
    row_chip,
    rows_near,
    row_far_out,
    rows_far,
    edge_in_sem,
    in_sem,
    small_in_sem,
    tile_send,
    tile_recv,
    edge_send,
    edge_recv,
    g_send,
    g_recv,
    bulk_send,
    bulk_recv,
    know,
    pair_send,
    pair_recv,
    near_send,
    near_recv,
    far_send,
    far_recv,
):
    S, L, W, n = dims
    blocks = W // ROWS
    reach = n // 8
    me = lax.axis_index("lon")
    core = lax.rem(me, 2)
    left, right = lax.rem(me + n - 1, n), lax.rem(me + 1, n)
    partner = me + 1 - 2 * core

    def away(distance):
        return lax.rem(me + distance + n, n)

    barrier = pltpu.get_barrier_semaphore()
    for to in (left, right):
        pl.semaphore_signal(barrier, inc=1, device_id={"lon": to}, device_id_type=MESH)

    load_edges = [
        pltpu.make_async_copy(tracer.at[:, :, blk], t_in.at[:, :, blk], edge_in_sem.at[i])
        for i, blk in enumerate((0, blocks - 1))
    ]
    load_off = pltpu.make_async_copy(offsets, off_in, small_in_sem.at[0])
    load_aa = pltpu.make_async_copy(air_after, aa_in, small_in_sem.at[1])
    load_ab = pltpu.make_async_copy(air_before, ab_in, small_in_sem.at[2])
    load_frac = pltpu.make_async_copy(frac, frac_in, small_in_sem.at[3])
    load_growth = pltpu.make_async_copy(growth, growth_in, small_in_sem.at[4])

    def load_inner(s):
        inner = pl.ds(1, blocks - 2)
        return pltpu.make_async_copy(tracer.at[s, :, inner], t_in.at[s, :, inner], in_sem.at[s])

    for copy in (*load_edges, load_off, load_aa, load_frac, load_ab, load_growth):
        copy.start()
    for s in range(S):
        load_inner(s).start()

    def remote(src, dst, send, recv, to):
        return pltpu.make_async_remote_copy(
            src_ref=src, dst_ref=dst, send_sem=send, recv_sem=recv, device_id={"lon": to}, device_id_type=MESH
        )

    tile_up = remote(tracer.at[0, :, blocks - 1], t_halo.at[0], tile_send.at[0], tile_recv.at[0], right)
    tile_down = remote(tracer.at[0, :, 0], t_halo.at[1], tile_send.at[1], tile_recv.at[1], left)
    others = pl.ds(1, S - 1)
    edge_up = remote(
        t_col.at[others, :, pl.ds(LOW + W - 1, 1)], t_col.at[others, :, pl.ds(LOW - 1, 1)], edge_send.at[0], edge_recv.at[0], right
    )
    edge_down = remote(
        t_col.at[others, :, pl.ds(LOW, 2)], t_col.at[others, :, pl.ds(LOW + W, 2)], edge_send.at[1], edge_recv.at[1], left
    )
    g_down = remote(g_out.at[0], g_halo.at[1], g_send.at[0], g_recv.at[0], left)
    g_up = remote(g_out.at[1], g_halo.at[0], g_send.at[1], g_recv.at[1], right)

    def bulk(s, sem, levels, up_count, down_first):
        down_count = HIGH - down_first
        return (
            remote(
                t_col.at[s, levels, pl.ds(W, up_count)],
                t_col.at[s, levels, pl.ds(0, up_count)],
                bulk_send.at[0, sem],
                bulk_recv.at[0, sem],
                right,
            ),
            remote(
                t_col.at[s, levels, pl.ds(LOW + down_first, down_count)],
                t_col.at[s, levels, pl.ds(LOW + W + down_first, down_count)],
                bulk_send.at[1, sem],
                bulk_recv.at[1, sem],
                left,
            ),
        )

    def bulk_first():
        return bulk(0, 0, pl.ds(0, L), LOW - ROWS, ROWS)

    def bulk_inner(s):
        return bulk(s, s, pl.ds(0, L), LOW - 1, 2)

    def bulk_last(lev):
        return bulk(S - 1, S - 1 + lev, pl.ds(lev, 1), LOW - 1, 2)

    steps = know_steps(1, 2 * reach + 1)
    rounds = len(steps)

    def tell(r):
        if r >= rounds:
            return
        for side, distance in ((0, steps[r]), (1, -steps[r])):
            pl.semaphore_signal(know.at[r, side], inc=1, device_id={"lon": away(distance)}, device_id_type=MESH)

    def hear(r):
        if r >= rounds:
            return
        for side in range(2):
            pl.semaphore_wait(know.at[r, side], 1)

    pl.semaphore_wait(barrier, 2)
    tile_up.start()
    tile_down.start()
    tell(0)

    for copy in load_edges:
        copy.wait()

    def relay_edges(s, _):
        for lev in range(L):
            for blk, l in ((0, 0), (0, 1), (blocks - 1, ROWS - 1)):
                t_col[s, lev, LOW + blk * ROWS + l] = t_in[s, lev, blk, pl.ds(l, ROWS, stride=ROWS), :]
        return 0

    lax.fori_loop(0, S, relay_edges, 0)
    edge_down.start()
    edge_up.start()
    load_off.wait()
    load_aa.wait()

    def relay_small(x, _):
        lev, blk = x // blocks, lax.rem(x, blocks)
        for l in range(ROWS):
            k_col[lev, blk * ROWS + l] = OFFMAX - off_in[lev, blk, pl.ds(l, ROWS, stride=ROWS), :]
            aa_col[lev, blk * ROWS + l] = aa_in[lev, blk, pl.ds(l, ROWS, stride=ROWS), :]
        return 0

    lax.fori_loop(0, L * blocks, relay_small, 0)

    def weight_of(lev, b):
        total = None
        for i in range(max(0, b - OFFMAX), min(W - 1, b + OFFMAX) + 1):
            term = jnp.where(k_col[lev, i] == OFFMAX - i + b, aa_col[lev, i], 0.0)
            total = term if total is None else total + term
        return total

    def g_sides(lev, _):
        for j in range(OFFMAX):
            g_out[0, lev, j] = weight_of(lev, j - OFFMAX)
            g_out[1, lev, j] = weight_of(lev, W + j)
        return 0

    lax.fori_loop(0, L, g_sides, 0)
    load_frac.wait()
    for lev in range(L):
        for j in range(ROWS):
            weight[0, lev, j : j + 1, :] = frac_in[lev : lev + 1, j * LANES : (j + 1) * LANES]
        for tap, w in enumerate(cubic_weights(weight[0, lev])):
            weight[tap, lev] = w
    g_down.start()
    g_up.start()
    hear(0)
    tell(1)
    load_ab.wait()

    def relay_before(x, _):
        lev, blk = x // blocks, lax.rem(x, blocks)
        for l in range(ROWS):
            ab_col[lev, blk * ROWS + l] = ab_in[lev, blk, pl.ds(l, ROWS, stride=ROWS), :]
        return 0

    lax.fori_loop(0, L * blocks, relay_before, 0)

    zero = jnp.zeros((ROWS, LANES), jnp.float32)

    def relay_species(s, _):
        load_inner(s).wait()

        def relay(lev, totals):
            totals = list(totals)
            for i in range(W):
                blk, l = divmod(i, ROWS)
                if 2 <= i < W - 1:
                    value = t_in[s, lev, blk, pl.ds(l, ROWS, stride=ROWS), :]
                    t_col[s, lev, LOW + i] = value
                else:
                    value = t_col[s, lev, LOW + i]
                totals[i % 4] = totals[i % 4] + value * ab_col[lev, i]
            return tuple(totals)

        totals = lax.fori_loop(0, L, relay, (zero,) * 4)
        acc[s] = (totals[0] + totals[1]) + (totals[2] + totals[3])
        return 0

    lax.fori_loop(0, S, relay_species, 0)
    for copy in bulk_first():
        copy.start()

    def send_bulk(s, _):
        for copy in bulk_inner(s):
            copy.start()
        return 0

    lax.fori_loop(1, S - 1, send_bulk, 0)
    for lev in range(L):
        for copy in bulk_last(lev):
            copy.start()
    hear(1)
    tell(2)

    def g_inside(lev, _):
        for b in range(W):
            g_col[lev, b] = weight_of(lev, b)
        return 0

    lax.fori_loop(0, L, g_inside, 0)

    def departures(s, lev, first, count):
        w = [weight[tap, lev] for tap in range(4)]
        t = [t_col[s, lev, LOW + first - 1 + j] for j in range(count + 3)]
        values = []
        for j in range(count):
            cubic = w[0] * t[j] + w[1] * t[j + 1]
            cubic = cubic + w[2] * t[j + 2] + w[3] * t[j + 3]
            low, high = jnp.minimum(t[j + 1], t[j + 2]), jnp.maximum(t[j + 1], t[j + 2])
            values.append(jnp.minimum(jnp.maximum(cubic, low), high))
            f_col[s, lev, OFFMAX + first + j] = values[-1]
        return values

    def inside(s, _):
        def level(lev, totals):
            totals = list(totals)
            for first in range(1, W - 2, ROWS):
                for j, value in enumerate(departures(s, lev, first, min(ROWS, W - 2 - first))):
                    totals[j % 4] = totals[j % 4] + value * g_col[lev, first + j]
            return tuple(totals)

        totals = lax.fori_loop(0, L, level, (zero,) * 4)
        acc[S + s] = (totals[0] + totals[1]) + (totals[2] + totals[3])
        return 0

    lax.fori_loop(0, S // 2, inside, 0)
    hear(2)
    tell(3)
    lax.fori_loop(S // 2, S, inside, 0)

    tile_up.wait_recv()
    tile_down.wait_recv()

    def relay_tiles(lev, _):
        for l in range(ROWS):
            rows = pl.ds(l, ROWS, stride=ROWS)
            t_col[0, lev, LOW - ROWS + l] = t_halo[0, lev, rows, :]
            t_col[0, lev, LOW + W + l] = t_halo[1, lev, rows, :]
        return 0

    lax.fori_loop(0, L, relay_tiles, 0)
    edge_up.wait_recv()
    edge_down.wait_recv()
    g_down.wait_recv()
    g_up.wait_recv()

    def outer_mass(lev, totals):
        g_low = [g_halo[0, lev, j] for j in range(OFFMAX)]
        g_high = [g_halo[1, lev, j] for j in range(OFFMAX)]
        sums = []
        for s in range(S):
            parts = [totals[s], zero]
            (first,) = departures(s, lev, 0, 1)
            last = departures(s, lev, W - 2, 2)
            parts[0] = parts[0] + first * g_col[lev, 0]
            parts[1] = parts[1] + last[0] * g_col[lev, W - 2]
            parts[1] = parts[1] + last[1] * g_col[lev, W - 1]
            for j in range(OFFMAX):
                low = first if j == 0 else f_col[s, lev, OFFMAX + j]
                at = W - OFFMAX + j
                high = last[at - W + 2] if at >= W - 2 else f_col[s, lev, OFFMAX + at]
                parts[0] = parts[0] + low * g_low[j]
                parts[1] = parts[1] + high * g_high[j]
            sums.append(parts[0] + parts[1])
        return tuple(sums)

    totals = lax.fori_loop(0, L, outer_mass, tuple(acc[S + s] for s in range(S)))
    for s in range(S):
        acc[S + s] = totals[s]

    sums = jnp.sum(jnp.sum(acc[...], axis=1), axis=1, keepdims=True)
    at_row = lax.broadcasted_iota(jnp.int32, (2 * S, LANES), 0)
    at_lane = lax.broadcasted_iota(jnp.int32, (2 * S, LANES), 1)
    row_own[...] = jnp.sum(jnp.where(at_row == at_lane, sums, 0.0), axis=0, keepdims=True)

    pair = remote(row_own, row_pair, pair_send.at[0], pair_recv.at[0], partner)
    pair.start()
    hear(3)
    tell(4)
    pair.wait_recv()
    row_chip[...] = row_own[...] + row_pair[...]
    for r in range(4, rounds):
        hear(r)
        tell(r + 1)

    way = 2 * (1 - 2 * core)

    def to_chip(d, at):
        return away(way * d - core + at)

    near = [
        remote(row_chip, rows_near.at[core, d], near_send.at[at, d], near_recv.at[core, d], to_chip(d + 1, at))
        for d in range(reach)
        for at in range(2)
    ]
    for copy in near:
        copy.start()

    def near_from(side, d):
        return remote(row_chip, rows_near.at[side, d], near_send.at[0, d], near_recv.at[side, d], partner)

    def halo(s, lev):
        for first in (-OFFMAX, -OFFMAX + 6, W, W + 6):
            departures(s, lev, first, 6)

    def gather(s, lev, blk):
        base = blk * ROWS
        f = [f_col[s, lev, base + j] for j in range(ROWS + 2 * OFFMAX)]
        for l in range(ROWS):
            k = k_col[lev, base + l]
            bits = [(k & (1 << bit)) != 0 for bit in range(5)]
            out[s, lev, blk, pl.ds(l, ROWS, stride=ROWS), :] = pick(bits, f[l : l + 2 * OFFMAX + 1])

    def level_cells(s, lev):
        def part(blk, _):
            gather(s, lev, blk)
            return 0

        halo(s, lev)
        lax.fori_loop(0, blocks, part, 0)

    def cells(s, copies):
        for copy in copies:
            copy.wait_recv()

        def level(lev, _):
            level_cells(s, lev)
            return 0

        lax.fori_loop(0, L, level, 0)

    def inner_cells(s, _):
        cells(s, bulk_inner(s))
        return 0

    early = max(1, S // 2 - 1)
    cells(0, bulk_first())
    lax.fori_loop(1, early, inner_cells, 0)

    for side in range(2):
        for d in range(reach):
            near_from(side, d).wait_recv()
    mine = jnp.sum(rows_near[core, pl.ds(0, reach - 1)], axis=0)
    row_far_out[...] = mine + jnp.where(core == 0, 1.0, 0.0) * rows_near[core, reach - 1]
    far = [
        remote(row_far_out, rows_far.at[core], far_send.at[at], far_recv.at[core], to_chip(reach, at)) for at in range(2)
    ]
    for copy in far:
        copy.start()
    near_total = row_chip[...] + jnp.sum(rows_near[0], axis=0) + jnp.sum(rows_near[1], axis=0)

    lax.fori_loop(early, S - 1, inner_cells, 0)
    for lev in range(L):
        for copy in bulk_last(lev):
            copy.wait_recv()
        level_cells(S - 1, lev)

    for side in range(2):
        remote(row_far_out, rows_far.at[side], far_send.at[0], far_recv.at[side], partner).wait_recv()
    load_growth.wait()
    total = near_total + (rows_far[0] + rows_far[1])
    spread = jnp.broadcast_to(total, (S, LANES))
    at_row = lax.broadcasted_iota(jnp.int32, (S, LANES), 0)
    at_lane = lax.broadcasted_iota(jnp.int32, (S, LANES), 1)
    before = jnp.sum(jnp.where(at_lane == at_row, spread, 0.0), axis=1, keepdims=True)
    after = jnp.sum(jnp.where(at_lane == at_row + S, spread, 0.0), axis=1, keepdims=True)
    gain = jnp.zeros((S, LANES), jnp.float32)
    for s in range(S):
        gain = jnp.where(at_row == s, 1.0 + growth_in[s], gain)
    ratio = before * gain / after
    for s in range(S):
        factor[s] = jnp.broadcast_to(ratio[s : s + 1, :], (ROWS, LANES))

    for copy in (tile_up, tile_down, edge_up, edge_down, g_down, g_up, pair, *near, *far, *bulk_first()):
        copy.wait_send()
    for lev in range(L):
        for copy in bulk_last(lev):
            copy.wait_send()

    def finish(s, _):
        for copy in bulk_inner(s):
            copy.wait_send()
        return 0

    lax.fori_loop(1, S - 1, finish, 0)


def scale_kernel(limited, factor, out, scaled, sem):
    S, L = limited.shape[:2]

    def put(s):
        return pltpu.make_async_copy(scaled.at[s], out.at[s], sem.at[s])

    def scale(s, _):
        gain = factor[s]

        def level(lev, _):
            for blk in range(limited.shape[2]):
                for row in range(0, limited.shape[3], ROWS):
                    scaled[s, lev, blk, pl.ds(row, ROWS), :] = limited[s, lev, blk, pl.ds(row, ROWS), :] * gain
            return 0

        lax.fori_loop(0, L, level, 0)
        put(s).start()
        return 0

    lax.fori_loop(0, S, scale, 0)
    for s in range(S):
        put(s).wait()


def to_tiles(a):
    *lead, cols, lats = a.shape
    k = len(lead)
    a = a.reshape(*lead, cols // ROWS, ROWS, lats // LANES, LANES)
    a = a.transpose(*range(k), k, k + 2, k + 1, k + 3)
    return a.reshape(*lead, cols // ROWS, lats // LANES * ROWS, LANES)


def from_tiles(a, cols, lats):
    *lead, _, _, _ = a.shape
    k = len(lead)
    a = a.reshape(*lead, cols // ROWS, lats // LANES, ROWS, LANES)
    a = a.transpose(*range(k), k, k + 2, k + 1, k + 3)
    return a.reshape(*lead, cols, lats)


def in_hbm(a):
    return pltpu.with_memory_space_constraint(a, pltpu.HBM)


def on_device(n, tracer, offsets, frac, air_before, air_after, growth):
    S, L, W, lats = tracer.shape
    tiles = to_tiles(tracer)
    f32, vmem = jnp.float32, pltpu.VMEM
    column = (ROWS, LANES)
    blocks = W // ROWS
    dma = pltpu.SemaphoreType.DMA
    reach = n // 8
    rounds = len(know_steps(1, 2 * reach + 1))
    small = (L, blocks, ROWS * ROWS, LANES)
    limited, factor = pl.pallas_call(
        functools.partial(kernel, (S, L, W, n)),
        out_shape=[pltpu.VMEM(tiles.shape, f32), pltpu.VMEM((S, *column), f32)],
        in_specs=[pl.BlockSpec(memory_space=pltpu.HBM)] * 6,

        out_specs=[pl.BlockSpec(memory_space=pltpu.VMEM)] * 2,
        scratch_shapes=[
            vmem(tiles.shape, f32),
            vmem((2, L, ROWS * ROWS, LANES), f32),
            vmem(frac.shape, f32),
            pltpu.SMEM(growth.shape, f32),
            vmem(small, jnp.int32),
            vmem(small, f32),
            vmem(small, f32),
            vmem((S, L, LOW + W + HIGH, *column), f32),
            vmem((L, W, *column), jnp.int32),
            vmem((L, W, *column), f32),
            vmem((L, W, *column), f32),
            vmem((L, W, *column), f32),
            vmem((2, L, OFFMAX, *column), f32),
            vmem((2, L, OFFMAX, *column), f32),
            vmem((S, L, W + 2 * OFFMAX, *column), f32),
            vmem((4, L, *column), f32),
            vmem((2 * S, *column), f32),
            vmem((1, LANES), f32),
            vmem((1, LANES), f32),
            vmem((1, LANES), f32),
            vmem((2, reach, 1, LANES), f32),
            vmem((1, LANES), f32),
            vmem((2, 1, LANES), f32),
            dma((2,)),
            dma((S,)),
            dma((5,)),
            dma((2,)),
            dma((2,)),
            dma((2,)),
            dma((2,)),
            dma((2,)),
            dma((2,)),
            dma((2, S - 1 + L)),
            dma((2, S - 1 + L)),
            pltpu.SemaphoreType.REGULAR((rounds, 2)),
            dma((1,)),
            dma((1,)),
            dma((2, reach)),
            dma((2, reach)),
            dma((2,)),
            dma((2,)),
        ],
        compiler_params=pltpu.CompilerParams(collective_id=0, has_side_effects=True, vmem_limit_bytes=44 * 2**20),
    )(*map(in_hbm, (tiles, to_tiles(offsets), to_tiles(air_before), to_tiles(air_after), frac, growth)))
    result = pl.pallas_call(
        scale_kernel,
        out_shape=jax.ShapeDtypeStruct(tiles.shape, f32),
        in_specs=[pl.BlockSpec(memory_space=pltpu.VMEM)] * 2,
        out_specs=pl.BlockSpec(memory_space=pl.ANY),
        scratch_shapes=[vmem(tiles.shape, f32), dma((S,))],
        compiler_params=pltpu.CompilerParams(vmem_limit_bytes=24 * 2**20),
    )(limited, factor)
    return from_tiles(result, W, lats)


def solution(mesh):
    placed = (
        P("scen", None, "lon", None),
        P(None, "lon", None),
        P(),
        P(None, "lon", None),
        P(None, "lon", None),
        P("scen"),
    )
    return jax.shard_map(
        functools.partial(on_device, mesh.shape["lon"]),
        mesh=mesh,
        in_specs=placed,
        out_specs=P("scen", None, "lon", None),
        check_vma=False,
    )
```

```python
import functools

import jax
import jax.numpy as jnp
from jax import lax
from jax.experimental import pallas as pl
from jax.experimental.pallas import tpu as pltpu
from jax.sharding import PartitionSpec as P

OFFMAX = 12
LANES = 128
ROWS = 8
LOW = OFFMAX + 1
HIGH = OFFMAX + 2
MESH = pl.DeviceIdType.MESH


def know_steps(known, wanted):
    steps = []
    while known < wanted:
        steps.append(min(known, wanted - known))
        known += steps[-1]
    return steps


def cubic_weights(fraction):
    first = -fraction * (1.0 - fraction) * (2.0 - fraction) / 6.0
    second = (1.0 + fraction) * (1.0 - fraction) * (2.0 - fraction) / 2.0
    third = (1.0 + fraction) * fraction * (2.0 - fraction) / 2.0
    fourth = -(1.0 + fraction) * fraction * (1.0 - fraction) / 6.0
    return (first, second, third, fourth)


def pick(bits, items):
    for bit in bits:
        merged = [jnp.where(bit, items[j + 1], items[j]) for j in range(0, len(items) - 1, 2)]
        if len(items) % 2:
            merged.append(items[-1])
        items = merged
    return items[0]


def kernel(
    dims,
    tracer,
    offsets,
    air_before,
    air_after,
    frac,
    growth,
    out,
    factor,
    t_in,
    t_halo,
    frac_in,
    growth_in,
    off_in,
    ab_in,
    aa_in,
    t_col,
    k_col,
    ab_col,
    aa_col,
    g_col,
    g_out_down,
    g_out_up,
    g_low,
    g_high,
    f_col,
    weight,
    acc,
    row_own,
    row_pair,
    row_chip,
    rows_near,
    row_far_out,
    rows_far,
    edge_in_sem,
    in_sem,
    small_in_sem,
    tile_send,
    tile_recv,
    edge_send,
    edge_recv,
    g_send,
    g_recv,
    bulk_send,
    bulk_recv,
    know,
    pair_send,
    pair_recv,
    near_send,
    near_recv,
    far_send,
    far_recv,
):
    S, L, W, n = dims
    blocks = W // ROWS
    reach = n // 8
    me = lax.axis_index("lon")
    core = lax.rem(me, 2)
    left, right = lax.rem(me + n - 1, n), lax.rem(me + 1, n)
    partner = me + 1 - 2 * core

    def away(distance):
        return lax.rem(me + distance + n, n)

    barrier = pltpu.get_barrier_semaphore()
    for to in (left, right):
        pl.semaphore_signal(barrier, inc=1, device_id={"lon": to}, device_id_type=MESH)

    load_edges = [
        pltpu.make_async_copy(tracer.at[:, :, blk], t_in.at[:, :, blk], edge_in_sem.at[i])
        for i, blk in enumerate((0, blocks - 1))
    ]
    load_off = pltpu.make_async_copy(offsets, off_in, small_in_sem.at[0])
    load_aa = pltpu.make_async_copy(air_after, aa_in, small_in_sem.at[1])
    load_ab = pltpu.make_async_copy(air_before, ab_in, small_in_sem.at[2])
    load_frac = pltpu.make_async_copy(frac, frac_in, small_in_sem.at[3])
    load_growth = pltpu.make_async_copy(growth, growth_in, small_in_sem.at[4])

    def load_inner(s):
        inner = pl.ds(1, blocks - 2)
        return pltpu.make_async_copy(tracer.at[s, :, inner], t_in.at[s, :, inner], in_sem.at[s])

    for copy in (*load_edges, load_off, load_aa, load_frac, load_ab, load_growth):
        copy.start()
    for s in range(S):
        load_inner(s).start()

    def remote(src, dst, send, recv, to):
        return pltpu.make_async_remote_copy(
            src_ref=src, dst_ref=dst, send_sem=send, recv_sem=recv, device_id={"lon": to}, device_id_type=MESH
        )

    tile_up = remote(tracer.at[0, :, blocks - 1], t_halo.at[0], tile_send.at[0], tile_recv.at[0], right)
    tile_down = remote(tracer.at[0, :, 0], t_halo.at[1], tile_send.at[1], tile_recv.at[1], left)
    half = S // 2

    def edge(species, count, source, target, sem, to):
        return remote(
            t_col.at[species, :, pl.ds(source, count)], t_col.at[species, :, pl.ds(target, count)], edge_send.at[sem], edge_recv.at[sem], to
        )

    one_half, other_half = pl.ds(1, half - 1), pl.ds(half, S - half)
    edges = [
        edge(one_half, 2, LOW, LOW + W, 0, left),
        edge(one_half, 1, LOW + W - 1, LOW - 1, 1, right),
        edge(other_half, 2, LOW + W - 2, LOW - 2, 2, right),
        edge(other_half, 1, LOW, LOW + W, 3, left),
    ]
    g_down = remote(g_out_down, g_high, g_send.at[0], g_recv.at[0], left)
    g_up = remote(g_out_up, g_low, g_send.at[1], g_recv.at[1], right)

    def bulk(s, sem, levels, up_count, down_first):
        down_count = HIGH - down_first
        return (
            remote(
                t_col.at[s, levels, pl.ds(W, up_count)],
                t_col.at[s, levels, pl.ds(0, up_count)],
                bulk_send.at[0, sem],
                bulk_recv.at[0, sem],
                right,
            ),
            remote(
                t_col.at[s, levels, pl.ds(LOW + down_first, down_count)],
                t_col.at[s, levels, pl.ds(LOW + W + down_first, down_count)],
                bulk_send.at[1, sem],
                bulk_recv.at[1, sem],
                left,
            ),
        )

    def bulk_first():
        return bulk(0, 0, pl.ds(0, L), LOW - ROWS, ROWS)

    def bulk_one(s):
        return bulk(s, s, pl.ds(0, L), LOW - 1, 2)

    def bulk_other(s):
        return bulk(s, s, pl.ds(0, L), LOW - 2, 1)

    def bulk_last(lev):
        return bulk(S - 1, S - 1 + lev, pl.ds(lev, 1), LOW - 2, 1)

    steps = know_steps(1, 2 * reach + 1)
    rounds = len(steps)

    def tell(r):
        if r >= rounds:
            return
        for side, distance in ((0, steps[r]), (1, -steps[r])):
            pl.semaphore_signal(know.at[r, side], inc=1, device_id={"lon": away(distance)}, device_id_type=MESH)

    def hear(r):
        if r >= rounds:
            return
        for side in range(2):
            pl.semaphore_wait(know.at[r, side], 1)

    pl.semaphore_wait(barrier, 2)
    tile_up.start()
    tile_down.start()
    tell(0)

    for copy in load_edges:
        copy.wait()

    def relay_edges(s, _):
        for lev in range(L):
            for blk, l in ((0, 0), (0, 1), (blocks - 1, ROWS - 2), (blocks - 1, ROWS - 1)):
                t_col[s, lev, LOW + blk * ROWS + l] = t_in[s, lev, blk, pl.ds(l, ROWS, stride=ROWS), :]
        return 0

    lax.fori_loop(0, S, relay_edges, 0)
    for copy in edges:
        copy.start()
    hear(0)
    tell(1)
    load_off.wait()
    load_aa.wait()

    def relay_small(x, _):
        lev, blk = x // blocks, lax.rem(x, blocks)
        for l in range(ROWS):
            k_col[lev, blk * ROWS + l] = OFFMAX - off_in[lev, blk, pl.ds(l, ROWS, stride=ROWS), :]
            aa_col[lev, blk * ROWS + l] = aa_in[lev, blk, pl.ds(l, ROWS, stride=ROWS), :]
        return 0

    lax.fori_loop(0, L * blocks, relay_small, 0)

    def weight_of(lev, b):
        total = None
        for i in range(max(0, b - OFFMAX), min(W - 1, b + OFFMAX) + 1):
            term = jnp.where(k_col[lev, i] == OFFMAX - i + b, aa_col[lev, i], 0.0)
            total = term if total is None else total + term
        return total

    def g_sides(lev, _):
        for j in range(OFFMAX):
            g_out_down[lev, j] = weight_of(lev, j - OFFMAX)
        for j in range(OFFMAX + 1):
            g_out_up[lev, j] = weight_of(lev, W - 1 + j)
        return 0

    lax.fori_loop(0, L, g_sides, 0)
    load_frac.wait()
    for lev in range(L):
        for j in range(ROWS):
            weight[0, lev, j : j + 1, :] = frac_in[lev : lev + 1, j * LANES : (j + 1) * LANES]
        for tap, w in enumerate(cubic_weights(weight[0, lev])):
            weight[tap, lev] = w
    g_down.start()
    g_up.start()
    load_ab.wait()

    def relay_before(x, _):
        lev, blk = x // blocks, lax.rem(x, blocks)
        for l in range(ROWS):
            ab_col[lev, blk * ROWS + l] = ab_in[lev, blk, pl.ds(l, ROWS, stride=ROWS), :]
        return 0

    lax.fori_loop(0, L * blocks, relay_before, 0)

    zero = jnp.zeros((ROWS, LANES), jnp.float32)

    def relay_species(s, _):
        load_inner(s).wait()

        def relay(lev, totals):
            totals = list(totals)
            for i in range(W):
                blk, l = divmod(i, ROWS)
                if 2 <= i < W - 2:
                    value = t_in[s, lev, blk, pl.ds(l, ROWS, stride=ROWS), :]
                    t_col[s, lev, LOW + i] = value
                else:
                    value = t_col[s, lev, LOW + i]
                totals[i % 4] = totals[i % 4] + value * ab_col[lev, i]
            return tuple(totals)

        totals = lax.fori_loop(0, L, relay, (zero,) * 4)
        acc[s] = (totals[0] + totals[1]) + (totals[2] + totals[3])
        return 0

    lax.fori_loop(0, half, relay_species, 0)
    hear(1)
    tell(2)
    lax.fori_loop(half, S, relay_species, 0)
    for copy in bulk_first():
        copy.start()

    def send_one(s, _):
        for copy in bulk_one(s):
            copy.start()
        return 0

    def send_other(s, _):
        for copy in bulk_other(s):
            copy.start()
        return 0

    lax.fori_loop(1, half, send_one, 0)
    lax.fori_loop(half, S - 1, send_other, 0)
    for lev in range(L):
        for copy in bulk_last(lev):
            copy.start()

    def g_inside(lev, _):
        for b in range(W - 1):
            g_col[lev, b] = weight_of(lev, b)
        g_col[lev, W - 1] = g_out_up[lev, 0]
        return 0

    lax.fori_loop(0, L, g_inside, 0)
    hear(2)
    tell(3)

    def departures(s, lev, first, count):
        w = [weight[tap, lev] for tap in range(4)]
        t = [t_col[s, lev, LOW + first - 1 + j] for j in range(count + 3)]
        values = []
        for j in range(count):
            cubic = w[0] * t[j] + w[1] * t[j + 1]
            cubic = cubic + w[2] * t[j + 2] + w[3] * t[j + 3]
            low, high = jnp.minimum(t[j + 1], t[j + 2]), jnp.maximum(t[j + 1], t[j + 2])
            values.append(jnp.minimum(jnp.maximum(cubic, low), high))
            f_col[s, lev, OFFMAX + first + j] = values[-1]
        return values

    def inside(s, _):
        def level(lev, totals):
            totals = list(totals)
            for first in range(1, W - 2, ROWS):
                for j, value in enumerate(departures(s, lev, first, min(ROWS, W - 2 - first))):
                    totals[j % 4] = totals[j % 4] + value * g_col[lev, first + j]
            return tuple(totals)

        totals = lax.fori_loop(0, L, level, (zero,) * 4)
        acc[S + s] = (totals[0] + totals[1]) + (totals[2] + totals[3])
        return 0

    lax.fori_loop(0, S, inside, 0)
    hear(3)
    tell(4)

    tile_up.wait_recv()
    tile_down.wait_recv()

    def relay_tiles(lev, _):
        for l in range(ROWS):
            rows = pl.ds(l, ROWS, stride=ROWS)
            t_col[0, lev, LOW - ROWS + l] = t_halo[0, lev, rows, :]
            t_col[0, lev, LOW + W + l] = t_halo[1, lev, rows, :]
        return 0

    lax.fori_loop(0, L, relay_tiles, 0)
    for copy in edges:
        copy.wait_recv()
    g_down.wait_recv()
    g_up.wait_recv()

    def outer_mass(lev, totals):
        low = [g_low[lev, j] for j in range(OFFMAX + 1)]
        high = [g_high[lev, j] for j in range(OFFMAX)]
        low[0] = low[0] + g_out_down[lev, OFFMAX - 1]
        low[1] = low[1] + g_col[lev, 0]
        high[OFFMAX - 2] = high[OFFMAX - 2] + g_col[lev, W - 2]
        high[OFFMAX - 1] = high[OFFMAX - 1] + g_col[lev, W - 1]
        sums = []
        for s in range(S):
            parts = [totals[s], zero]
            if s < half:
                first, last = departures(s, lev, 0, 1), departures(s, lev, W - 2, 2)
            else:
                first, last = departures(s, lev, -1, 2), departures(s, lev, W - 2, 1)
            near_low = [(first[-1], low[1])] + [(f_col[s, lev, OFFMAX + j], low[1 + j]) for j in range(1, OFFMAX)]
            if s >= half:
                near_low.append((first[0], low[0]))
            near_high = [(f_col[s, lev, W + j], high[j]) for j in range(OFFMAX - 2)]
            near_high += [(value, high[OFFMAX - 2 + j]) for j, value in enumerate(last)]
            for i, pairs in enumerate((near_low, near_high)):
                for value, mass in pairs:
                    parts[i] = parts[i] + value * mass
            sums.append(parts[0] + parts[1])
        return tuple(sums)

    totals = lax.fori_loop(0, L, outer_mass, tuple(acc[S + s] for s in range(S)))
    for s in range(S):
        acc[S + s] = totals[s]

    sums = jnp.sum(jnp.sum(acc[...], axis=1), axis=1, keepdims=True)
    at_row = lax.broadcasted_iota(jnp.int32, (2 * S, LANES), 0)
    at_lane = lax.broadcasted_iota(jnp.int32, (2 * S, LANES), 1)
    row_own[...] = jnp.sum(jnp.where(at_row == at_lane, sums, 0.0), axis=0, keepdims=True)

    pair = remote(row_own, row_pair, pair_send.at[0], pair_recv.at[0], partner)
    pair.start()
    pair.wait_recv()
    row_chip[...] = row_own[...] + row_pair[...]
    for r in range(4, rounds):
        hear(r)
        tell(r + 1)

    way = 2 * (1 - 2 * core)

    def to_chip(d, at):
        return away(way * d - core + at)

    near = [
        [remote(row_chip, rows_near.at[core, d], near_send.at[at, d], near_recv.at[core, d], to_chip(d + 1, at)) for at in range(2)]
        for d in range(reach)
    ]
    for d in range(reach - 1):
        for copy in near[d]:
            copy.start()

    @pl.when(core == 1)
    def _():
        for copy in near[reach - 1]:
            copy.start()

    def near_from(side, d):
        return remote(row_chip, rows_near.at[side, d], near_send.at[0, d], near_recv.at[side, d], partner)

    def halo(s, lev):
        for first, count in ((-OFFMAX, 6), (-OFFMAX + 6, 6), (W - 1, 7), (W + 6, 6)):
            departures(s, lev, first, count)

    def gather(s, lev, blk):
        base = blk * ROWS
        f = [f_col[s, lev, base + j] for j in range(ROWS + 2 * OFFMAX)]
        for l in range(ROWS):
            k = k_col[lev, base + l]
            bits = [(k & (1 << bit)) != 0 for bit in range(5)]
            out[s, lev, blk, pl.ds(l, ROWS, stride=ROWS), :] = pick(bits, f[l : l + 2 * OFFMAX + 1])

    def level_cells(s, lev):
        def part(blk, _):
            gather(s, lev, blk)
            return 0

        halo(s, lev)
        lax.fori_loop(0, blocks, part, 0)

    def cells(s, copies):
        for copy in copies:
            copy.wait_recv()

        def level(lev, _):
            level_cells(s, lev)
            return 0

        lax.fori_loop(0, L, level, 0)

    def one_cells(s, _):
        cells(s, bulk_one(s))
        return 0

    def other_cells(s, _):
        cells(s, bulk_other(s))
        return 0

    early = max(1, half - 1)
    cells(0, bulk_first())
    lax.fori_loop(1, early, one_cells, 0)

    for d in range(reach - 1):
        near_from(core, d).wait_recv()
    mine = jnp.sum(rows_near[core, pl.ds(0, reach - 1)], axis=0)

    @pl.when(core == 0)
    def _():
        row_far_out[...] = mine + row_chip[...]

    @pl.when(core == 1)
    def _():
        near_from(1, reach - 1).wait_recv()
        row_far_out[...] = mine + rows_near[1, reach - 1]

    far = [
        remote(row_far_out, rows_far.at[core], far_send.at[at], far_recv.at[core], to_chip(reach, at)) for at in range(2)
    ]
    for copy in far:
        copy.start()
    for d in range(reach - 1):
        near_from(1 - core, d).wait_recv()

    @pl.when(core == 0)
    def _():
        near_from(1, reach - 1).wait_recv()

    near_total = row_chip[...] + jnp.sum(rows_near[0, pl.ds(0, reach - 1)], axis=0) + jnp.sum(rows_near[1], axis=0)

    lax.fori_loop(early, half, one_cells, 0)
    lax.fori_loop(half, S - 1, other_cells, 0)
    for lev in range(L):
        for copy in bulk_last(lev):
            copy.wait_recv()
        level_cells(S - 1, lev)

    for side in range(2):
        remote(row_far_out, rows_far.at[side], far_send.at[0], far_recv.at[side], partner).wait_recv()
    load_growth.wait()
    total = near_total + (rows_far[0] + rows_far[1])
    spread = jnp.broadcast_to(total, (S, LANES))
    at_row = lax.broadcasted_iota(jnp.int32, (S, LANES), 0)
    at_lane = lax.broadcasted_iota(jnp.int32, (S, LANES), 1)
    before = jnp.sum(jnp.where(at_lane == at_row, spread, 0.0), axis=1, keepdims=True)
    after = jnp.sum(jnp.where(at_lane == at_row + S, spread, 0.0), axis=1, keepdims=True)
    gain = jnp.zeros((S, LANES), jnp.float32)
    for s in range(S):
        gain = jnp.where(at_row == s, 1.0 + growth_in[s], gain)
    ratio = before * gain / after
    for s in range(S):
        factor[s] = jnp.broadcast_to(ratio[s : s + 1, :], (ROWS, LANES))

    for copy in (tile_up, tile_down, *edges, g_down, g_up, pair, *sum(near[:-1], []), *far, *bulk_first()):
        copy.wait_send()

    @pl.when(core == 1)
    def _():
        for copy in near[reach - 1]:
            copy.wait_send()

    for lev in range(L):
        for copy in bulk_last(lev):
            copy.wait_send()

    def finish_one(s, _):
        for copy in bulk_one(s):
            copy.wait_send()
        return 0

    def finish_other(s, _):
        for copy in bulk_other(s):
            copy.wait_send()
        return 0

    lax.fori_loop(1, half, finish_one, 0)
    lax.fori_loop(half, S - 1, finish_other, 0)


def scale_kernel(limited, factor, out, scaled, sem):
    S, L = limited.shape[:2]

    def put(s):
        return pltpu.make_async_copy(scaled.at[s], out.at[s], sem.at[s])

    def scale(s, _):
        gain = factor[s]

        def level(lev, _):
            for blk in range(limited.shape[2]):
                for row in range(0, limited.shape[3], ROWS):
                    scaled[s, lev, blk, pl.ds(row, ROWS), :] = limited[s, lev, blk, pl.ds(row, ROWS), :] * gain
            return 0

        lax.fori_loop(0, L, level, 0)
        put(s).start()
        return 0

    lax.fori_loop(0, S, scale, 0)
    for s in range(S):
        put(s).wait()


def to_tiles(a):
    *lead, cols, lats = a.shape
    k = len(lead)
    a = a.reshape(*lead, cols // ROWS, ROWS, lats // LANES, LANES)
    a = a.transpose(*range(k), k, k + 2, k + 1, k + 3)
    return a.reshape(*lead, cols // ROWS, lats // LANES * ROWS, LANES)


def from_tiles(a, cols, lats):
    *lead, _, _, _ = a.shape
    k = len(lead)
    a = a.reshape(*lead, cols // ROWS, lats // LANES, ROWS, LANES)
    a = a.transpose(*range(k), k, k + 2, k + 1, k + 3)
    return a.reshape(*lead, cols, lats)


def in_hbm(a):
    return pltpu.with_memory_space_constraint(a, pltpu.HBM)


def on_device(n, tracer, offsets, frac, air_before, air_after, growth):
    S, L, W, lats = tracer.shape
    tiles = to_tiles(tracer)
    f32, vmem = jnp.float32, pltpu.VMEM
    column = (ROWS, LANES)
    blocks = W // ROWS
    dma = pltpu.SemaphoreType.DMA
    reach = n // 8
    rounds = len(know_steps(1, 2 * reach + 1))
    small = (L, blocks, ROWS * ROWS, LANES)
    limited, factor = pl.pallas_call(
        functools.partial(kernel, (S, L, W, n)),
        out_shape=[pltpu.VMEM(tiles.shape, f32), pltpu.VMEM((S, *column), f32)],
        in_specs=[pl.BlockSpec(memory_space=pltpu.HBM)] * 6,

        out_specs=[pl.BlockSpec(memory_space=pltpu.VMEM)] * 2,
        scratch_shapes=[
            vmem(tiles.shape, f32),
            vmem((2, L, ROWS * ROWS, LANES), f32),
            vmem(frac.shape, f32),
            pltpu.SMEM(growth.shape, f32),
            vmem(small, jnp.int32),
            vmem(small, f32),
            vmem(small, f32),
            vmem((S, L, LOW + W + HIGH, *column), f32),
            vmem((L, W, *column), jnp.int32),
            vmem((L, W, *column), f32),
            vmem((L, W, *column), f32),
            vmem((L, W, *column), f32),
            vmem((L, OFFMAX, *column), f32),
            vmem((L, OFFMAX + 1, *column), f32),
            vmem((L, OFFMAX + 1, *column), f32),
            vmem((L, OFFMAX, *column), f32),
            vmem((S, L, W + 2 * OFFMAX, *column), f32),
            vmem((4, L, *column), f32),
            vmem((2 * S, *column), f32),
            vmem((1, LANES), f32),
            vmem((1, LANES), f32),
            vmem((1, LANES), f32),
            vmem((2, reach, 1, LANES), f32),
            vmem((1, LANES), f32),
            vmem((2, 1, LANES), f32),
            dma((2,)),
            dma((S,)),
            dma((5,)),
            dma((2,)),
            dma((2,)),
            dma((4,)),
            dma((4,)),
            dma((2,)),
            dma((2,)),
            dma((2, S - 1 + L)),
            dma((2, S - 1 + L)),
            pltpu.SemaphoreType.REGULAR((rounds, 2)),
            dma((1,)),
            dma((1,)),
            dma((2, reach)),
            dma((2, reach)),
            dma((2,)),
            dma((2,)),
        ],
        compiler_params=pltpu.CompilerParams(collective_id=0, has_side_effects=True, vmem_limit_bytes=44 * 2**20),
    )(*map(in_hbm, (tiles, to_tiles(offsets), to_tiles(air_before), to_tiles(air_after), frac, growth)))
    result = pl.pallas_call(
        scale_kernel,
        out_shape=jax.ShapeDtypeStruct(tiles.shape, f32),
        in_specs=[pl.BlockSpec(memory_space=pltpu.VMEM)] * 2,
        out_specs=pl.BlockSpec(memory_space=pl.ANY),
        scratch_shapes=[vmem(tiles.shape, f32), dma((S,))],
        compiler_params=pltpu.CompilerParams(vmem_limit_bytes=24 * 2**20),
    )(limited, factor)
    return from_tiles(result, W, lats)


def solution(mesh):
    placed = (
        P("scen", None, "lon", None),
        P(None, "lon", None),
        P(),
        P(None, "lon", None),
        P(None, "lon", None),
        P("scen"),
    )
    return jax.shard_map(
        functools.partial(on_device, mesh.shape["lon"]),
        mesh=mesh,
        in_specs=placed,
        out_specs=P("scen", None, "lon", None),
        check_vma=False,
    )
```

```python
import functools

import jax
import jax.numpy as jnp
from jax import lax
from jax.experimental import pallas as pl
from jax.experimental.pallas import tpu as pltpu
from jax.sharding import PartitionSpec as P

OFFMAX = 12
LANES = 128
ROWS = 8
LOW = OFFMAX + 1
HIGH = OFFMAX + 2
MESH = pl.DeviceIdType.MESH


def know_steps(known, wanted):
    steps = []
    while known < wanted:
        steps.append(min(known, wanted - known))
        known += steps[-1]
    return steps


def cubic_weights(fraction):
    first = -fraction * (1.0 - fraction) * (2.0 - fraction) / 6.0
    second = (1.0 + fraction) * (1.0 - fraction) * (2.0 - fraction) / 2.0
    third = (1.0 + fraction) * fraction * (2.0 - fraction) / 2.0
    fourth = -(1.0 + fraction) * fraction * (1.0 - fraction) / 6.0
    return (first, second, third, fourth)


def pick(bits, items):
    for bit in bits:
        merged = [jnp.where(bit, items[j + 1], items[j]) for j in range(0, len(items) - 1, 2)]
        if len(items) % 2:
            merged.append(items[-1])
        items = merged
    return items[0]


def kernel(
    dims,
    tracer,
    offsets,
    air_before,
    air_after,
    frac,
    growth,
    out,
    factor,
    t_in,
    t_halo,
    frac_in,
    growth_in,
    off_in,
    ab_in,
    aa_in,
    t_col,
    k_col,
    ab_col,
    aa_col,
    g_col,
    g_out_down,
    g_out_up,
    g_low,
    g_high,
    f_col,
    weight,
    acc,
    row_own,
    row_pair,
    row_chip,
    rows_near,
    row_side,
    row_other,
    row_far_out,
    rows_far,
    edge_in_sem,
    in_sem,
    small_in_sem,
    tile_send,
    tile_recv,
    edge_send,
    edge_recv,
    g_send,
    g_recv,
    bulk_send,
    bulk_recv,
    know,
    pair_send,
    pair_recv,
    near_send,
    near_recv,
    far_send,
    far_recv,
):
    S, L, W, n = dims
    blocks = W // ROWS
    reach = n // 8
    me = lax.axis_index("lon")
    core = lax.rem(me, 2)
    left, right = lax.rem(me + n - 1, n), lax.rem(me + 1, n)
    partner = me + 1 - 2 * core

    def away(distance):
        return lax.rem(me + distance + n, n)

    barrier = pltpu.get_barrier_semaphore()
    for to in (left, right):
        pl.semaphore_signal(barrier, inc=1, device_id={"lon": to}, device_id_type=MESH)

    load_edges = [
        pltpu.make_async_copy(tracer.at[:, :, blk], t_in.at[:, :, blk], edge_in_sem.at[i])
        for i, blk in enumerate((0, blocks - 1))
    ]
    load_off = pltpu.make_async_copy(offsets, off_in, small_in_sem.at[0])
    load_aa = pltpu.make_async_copy(air_after, aa_in, small_in_sem.at[1])
    load_ab = pltpu.make_async_copy(air_before, ab_in, small_in_sem.at[2])
    load_frac = pltpu.make_async_copy(frac, frac_in, small_in_sem.at[3])
    load_growth = pltpu.make_async_copy(growth, growth_in, small_in_sem.at[4])

    def load_inner(s):
        inner = pl.ds(1, blocks - 2)
        return pltpu.make_async_copy(tracer.at[s, :, inner], t_in.at[s, :, inner], in_sem.at[s])

    for copy in (*load_edges, load_off, load_aa, load_frac, load_ab, load_growth):
        copy.start()
    for s in range(S):
        load_inner(s).start()

    def remote(src, dst, send, recv, to):
        return pltpu.make_async_remote_copy(
            src_ref=src, dst_ref=dst, send_sem=send, recv_sem=recv, device_id={"lon": to}, device_id_type=MESH
        )

    tile_up = remote(tracer.at[0, :, blocks - 1], t_halo.at[0], tile_send.at[0], tile_recv.at[0], right)
    tile_down = remote(tracer.at[0, :, 0], t_halo.at[1], tile_send.at[1], tile_recv.at[1], left)
    half = S // 2

    def edge(species, count, source, target, sem, to):
        return remote(
            t_col.at[species, :, pl.ds(source, count)], t_col.at[species, :, pl.ds(target, count)], edge_send.at[sem], edge_recv.at[sem], to
        )

    one_half, other_half = pl.ds(1, half - 1), pl.ds(half, S - half)
    edges = [
        edge(one_half, 2, LOW, LOW + W, 0, left),
        edge(one_half, 1, LOW + W - 1, LOW - 1, 1, right),
        edge(other_half, 2, LOW + W - 2, LOW - 2, 2, right),
        edge(other_half, 1, LOW, LOW + W, 3, left),
    ]
    g_down = remote(g_out_down, g_high, g_send.at[0], g_recv.at[0], left)
    g_up = remote(g_out_up, g_low, g_send.at[1], g_recv.at[1], right)

    def bulk(s, sem, levels, up_count, down_first):
        down_count = HIGH - down_first
        return (
            remote(
                t_col.at[s, levels, pl.ds(W, up_count)],
                t_col.at[s, levels, pl.ds(0, up_count)],
                bulk_send.at[0, sem],
                bulk_recv.at[0, sem],
                right,
            ),
            remote(
                t_col.at[s, levels, pl.ds(LOW + down_first, down_count)],
                t_col.at[s, levels, pl.ds(LOW + W + down_first, down_count)],
                bulk_send.at[1, sem],
                bulk_recv.at[1, sem],
                left,
            ),
        )

    def bulk_first():
        return bulk(0, 0, pl.ds(0, L), LOW - ROWS, ROWS)

    def bulk_one(s):
        return bulk(s, s, pl.ds(0, L), LOW - 1, 2)

    def bulk_other(s):
        return bulk(s, s, pl.ds(0, L), LOW - 2, 1)

    def bulk_last(lev):
        return bulk(S - 1, S - 1 + lev, pl.ds(lev, 1), LOW - 2, 1)

    steps = know_steps(1, 2 * reach + 1)
    rounds = len(steps)

    def tell(r):
        if r >= rounds:
            return
        for side, distance in ((0, steps[r]), (1, -steps[r])):
            pl.semaphore_signal(know.at[r, side], inc=1, device_id={"lon": away(distance)}, device_id_type=MESH)

    def hear(r):
        if r >= rounds:
            return
        for side in range(2):
            pl.semaphore_wait(know.at[r, side], 1)

    pl.semaphore_wait(barrier, 2)
    tile_up.start()
    tile_down.start()
    tell(0)

    for copy in load_edges:
        copy.wait()

    def relay_edges(s, _):
        for lev in range(L):
            for blk, l in ((0, 0), (0, 1), (blocks - 1, ROWS - 2), (blocks - 1, ROWS - 1)):
                t_col[s, lev, LOW + blk * ROWS + l] = t_in[s, lev, blk, pl.ds(l, ROWS, stride=ROWS), :]
        return 0

    lax.fori_loop(0, S, relay_edges, 0)
    for copy in edges:
        copy.start()
    hear(0)
    tell(1)
    load_off.wait()
    load_aa.wait()

    def relay_small(x, _):
        lev, blk = x // blocks, lax.rem(x, blocks)
        for l in range(ROWS):
            k_col[lev, blk * ROWS + l] = OFFMAX - off_in[lev, blk, pl.ds(l, ROWS, stride=ROWS), :]
            aa_col[lev, blk * ROWS + l] = aa_in[lev, blk, pl.ds(l, ROWS, stride=ROWS), :]
        return 0

    lax.fori_loop(0, L * blocks, relay_small, 0)

    def weight_of(lev, b):
        total = None
        for i in range(max(0, b - OFFMAX), min(W - 1, b + OFFMAX) + 1):
            term = jnp.where(k_col[lev, i] == OFFMAX - i + b, aa_col[lev, i], 0.0)
            total = term if total is None else total + term
        return total

    def g_sides(lev, _):
        for j in range(OFFMAX):
            g_out_down[lev, j] = weight_of(lev, j - OFFMAX)
        for j in range(OFFMAX + 1):
            g_out_up[lev, j] = weight_of(lev, W - 1 + j)
        return 0

    lax.fori_loop(0, L, g_sides, 0)
    load_frac.wait()
    for lev in range(L):
        for j in range(ROWS):
            weight[0, lev, j : j + 1, :] = frac_in[lev : lev + 1, j * LANES : (j + 1) * LANES]
        for tap, w in enumerate(cubic_weights(weight[0, lev])):
            weight[tap, lev] = w
    g_down.start()
    g_up.start()
    load_ab.wait()

    def relay_before(x, _):
        lev, blk = x // blocks, lax.rem(x, blocks)
        for l in range(ROWS):
            ab_col[lev, blk * ROWS + l] = ab_in[lev, blk, pl.ds(l, ROWS, stride=ROWS), :]
        return 0

    lax.fori_loop(0, L * blocks, relay_before, 0)

    zero = jnp.zeros((ROWS, LANES), jnp.float32)

    def relay_species(s, _):
        load_inner(s).wait()

        def relay(lev, totals):
            totals = list(totals)
            for i in range(W):
                blk, l = divmod(i, ROWS)
                if 2 <= i < W - 2:
                    value = t_in[s, lev, blk, pl.ds(l, ROWS, stride=ROWS), :]
                    t_col[s, lev, LOW + i] = value
                else:
                    value = t_col[s, lev, LOW + i]
                totals[i % 4] = totals[i % 4] + value * ab_col[lev, i]
            return tuple(totals)

        totals = lax.fori_loop(0, L, relay, (zero,) * 4)
        acc[s] = (totals[0] + totals[1]) + (totals[2] + totals[3])
        return 0

    lax.fori_loop(0, half, relay_species, 0)
    hear(1)
    tell(2)
    lax.fori_loop(half, S, relay_species, 0)
    for copy in bulk_first():
        copy.start()

    def send_one(s, _):
        for copy in bulk_one(s):
            copy.start()
        return 0

    def send_other(s, _):
        for copy in bulk_other(s):
            copy.start()
        return 0

    lax.fori_loop(1, half, send_one, 0)
    lax.fori_loop(half, S - 1, send_other, 0)
    for lev in range(L):
        for copy in bulk_last(lev):
            copy.start()

    def g_inside(lev, _):
        for b in range(W - 1):
            g_col[lev, b] = weight_of(lev, b)
        g_col[lev, W - 1] = g_out_up[lev, 0]
        return 0

    lax.fori_loop(0, L, g_inside, 0)
    hear(2)
    tell(3)

    def departures(s, lev, first, count):
        w = [weight[tap, lev] for tap in range(4)]
        t = [t_col[s, lev, LOW + first - 1 + j] for j in range(count + 3)]
        values = []
        for j in range(count):
            cubic = w[0] * t[j] + w[1] * t[j + 1]
            cubic = cubic + w[2] * t[j + 2] + w[3] * t[j + 3]
            low, high = jnp.minimum(t[j + 1], t[j + 2]), jnp.maximum(t[j + 1], t[j + 2])
            values.append(jnp.minimum(jnp.maximum(cubic, low), high))
            f_col[s, lev, OFFMAX + first + j] = values[-1]
        return values

    def inside(s, _):
        def level(lev, totals):
            totals = list(totals)
            for first in range(1, W - 2, ROWS):
                for j, value in enumerate(departures(s, lev, first, min(ROWS, W - 2 - first))):
                    totals[j % 4] = totals[j % 4] + value * g_col[lev, first + j]
            return tuple(totals)

        totals = lax.fori_loop(0, L, level, (zero,) * 4)
        acc[S + s] = (totals[0] + totals[1]) + (totals[2] + totals[3])
        return 0

    lax.fori_loop(0, S, inside, 0)
    hear(3)
    tell(4)

    tile_up.wait_recv()
    tile_down.wait_recv()

    def relay_tiles(lev, _):
        for l in range(ROWS):
            rows = pl.ds(l, ROWS, stride=ROWS)
            t_col[0, lev, LOW - ROWS + l] = t_halo[0, lev, rows, :]
            t_col[0, lev, LOW + W + l] = t_halo[1, lev, rows, :]
        return 0

    lax.fori_loop(0, L, relay_tiles, 0)
    for copy in edges:
        copy.wait_recv()
    g_down.wait_recv()
    g_up.wait_recv()

    def outer_mass(lev, totals):
        low = [g_low[lev, j] for j in range(OFFMAX + 1)]
        high = [g_high[lev, j] for j in range(OFFMAX)]
        low[0] = low[0] + g_out_down[lev, OFFMAX - 1]
        low[1] = low[1] + g_col[lev, 0]
        high[OFFMAX - 2] = high[OFFMAX - 2] + g_col[lev, W - 2]
        high[OFFMAX - 1] = high[OFFMAX - 1] + g_col[lev, W - 1]
        sums = []
        for s in range(S):
            parts = [totals[s], zero]
            if s < half:
                first, last = departures(s, lev, 0, 1), departures(s, lev, W - 2, 2)
            else:
                first, last = departures(s, lev, -1, 2), departures(s, lev, W - 2, 1)
            near_low = [(first[-1], low[1])] + [(f_col[s, lev, OFFMAX + j], low[1 + j]) for j in range(1, OFFMAX)]
            if s >= half:
                near_low.append((first[0], low[0]))
            near_high = [(f_col[s, lev, W + j], high[j]) for j in range(OFFMAX - 2)]
            near_high += [(value, high[OFFMAX - 2 + j]) for j, value in enumerate(last)]
            for i, pairs in enumerate((near_low, near_high)):
                for value, mass in pairs:
                    parts[i] = parts[i] + value * mass
            sums.append(parts[0] + parts[1])
        return tuple(sums)

    totals = lax.fori_loop(0, L, outer_mass, tuple(acc[S + s] for s in range(S)))
    for s in range(S):
        acc[S + s] = totals[s]

    sums = jnp.sum(jnp.sum(acc[...], axis=1), axis=1, keepdims=True)
    at_row = lax.broadcasted_iota(jnp.int32, (2 * S, LANES), 0)
    at_lane = lax.broadcasted_iota(jnp.int32, (2 * S, LANES), 1)
    row_own[...] = jnp.sum(jnp.where(at_row == at_lane, sums, 0.0), axis=0, keepdims=True)

    pair = remote(row_own, row_pair, pair_send.at[0], pair_recv.at[0], partner)
    pair.start()
    pair.wait_recv()
    row_chip[...] = row_own[...] + row_pair[...]
    for r in range(4, rounds):
        hear(r)
        tell(r + 1)

    way = 2 * (1 - 2 * core)
    near = [remote(row_chip, rows_near.at[d], near_send.at[d], near_recv.at[d], away(way * (d + 1))) for d in range(reach)]

    @pl.when(core == 1)
    def _():
        near[reach - 1].start()

    for copy in near[reach - 2 :: -1]:
        copy.start()

    def halo(s, lev):
        for first, count in ((-OFFMAX, 6), (-OFFMAX + 6, 6), (W - 1, 7), (W + 6, 6)):
            departures(s, lev, first, count)

    def gather(s, lev, blk):
        base = blk * ROWS
        f = [f_col[s, lev, base + j] for j in range(ROWS + 2 * OFFMAX)]
        for l in range(ROWS):
            k = k_col[lev, base + l]
            bits = [(k & (1 << bit)) != 0 for bit in range(5)]
            out[s, lev, blk, pl.ds(l, ROWS, stride=ROWS), :] = pick(bits, f[l : l + 2 * OFFMAX + 1])

    def level_cells(s, lev):
        def part(blk, _):
            gather(s, lev, blk)
            return 0

        halo(s, lev)
        lax.fori_loop(0, blocks, part, 0)

    def cells(s, copies):
        for copy in copies:
            copy.wait_recv()

        def level(lev, _):
            level_cells(s, lev)
            return 0

        lax.fori_loop(0, L, level, 0)

    def one_cells(s, _):
        cells(s, bulk_one(s))
        return 0

    def other_cells(s, _):
        cells(s, bulk_other(s))
        return 0

    early = max(1, half - 1)
    cells(0, bulk_first())
    lax.fori_loop(1, early, one_cells, 0)

    for copy in near[:-1]:
        copy.wait_recv()
    mine = jnp.sum(rows_near[pl.ds(0, reach - 1)], axis=0)

    @pl.when(core == 0)
    def _():
        row_far_out[...] = mine + row_chip[...]
        row_side[...] = mine

    @pl.when(core == 1)
    def _():
        near[reach - 1].wait_recv()
        row_far_out[...] = mine + rows_near[reach - 1]
        row_side[...] = mine + rows_near[reach - 1]

    far = [
        remote(row_far_out, rows_far.at[core], far_send.at[at], far_recv.at[core], away(way * reach - core + at)) for at in range(2)
    ]
    for copy in far:
        copy.start()
    swap = remote(row_side, row_other, pair_send.at[1], pair_recv.at[1], partner)
    swap.start()

    lax.fori_loop(early, half, one_cells, 0)
    lax.fori_loop(half, S - 1, other_cells, 0)
    def last_cells(lev):
        for copy in bulk_last(lev):
            copy.wait_recv()
        level_cells(S - 1, lev)

    for lev in range(L - 1):
        last_cells(lev)
    swap.wait_recv()
    for side in range(2):
        remote(row_far_out, rows_far.at[side], far_send.at[0], far_recv.at[side], partner).wait_recv()
    load_growth.wait()
    total = row_chip[...] + (row_side[...] + row_other[...]) + (rows_far[0] + rows_far[1])
    spread = jnp.broadcast_to(total, (S, LANES))
    at_row = lax.broadcasted_iota(jnp.int32, (S, LANES), 0)
    at_lane = lax.broadcasted_iota(jnp.int32, (S, LANES), 1)
    before = jnp.sum(jnp.where(at_lane == at_row, spread, 0.0), axis=1, keepdims=True)
    after = jnp.sum(jnp.where(at_lane == at_row + S, spread, 0.0), axis=1, keepdims=True)
    gain = jnp.zeros((S, LANES), jnp.float32)
    for s in range(S):
        gain = jnp.where(at_row == s, 1.0 + growth_in[s], gain)
    ratio = before * gain / after
    for s in range(S):
        factor[s] = jnp.broadcast_to(ratio[s : s + 1, :], (ROWS, LANES))

    last_cells(L - 1)

    for copy in (tile_up, tile_down, *edges, g_down, g_up, pair, swap, *near[:-1], *far, *bulk_first()):
        copy.wait_send()

    @pl.when(core == 1)
    def _():
        near[reach - 1].wait_send()

    for lev in range(L):
        for copy in bulk_last(lev):
            copy.wait_send()

    def finish_one(s, _):
        for copy in bulk_one(s):
            copy.wait_send()
        return 0

    def finish_other(s, _):
        for copy in bulk_other(s):
            copy.wait_send()
        return 0

    lax.fori_loop(1, half, finish_one, 0)
    lax.fori_loop(half, S - 1, finish_other, 0)


def scale_kernel(limited, factor, out, scaled, sem):
    S, L = limited.shape[:2]

    def put(s):
        return pltpu.make_async_copy(scaled.at[s], out.at[s], sem.at[s])

    def scale(s, _):
        gain = factor[s]

        def level(lev, _):
            for blk in range(limited.shape[2]):
                for row in range(0, limited.shape[3], ROWS):
                    scaled[s, lev, blk, pl.ds(row, ROWS), :] = limited[s, lev, blk, pl.ds(row, ROWS), :] * gain
            return 0

        lax.fori_loop(0, L, level, 0)
        put(s).start()
        return 0

    lax.fori_loop(0, S, scale, 0)
    for s in range(S):
        put(s).wait()


def to_tiles(a):
    *lead, cols, lats = a.shape
    k = len(lead)
    a = a.reshape(*lead, cols // ROWS, ROWS, lats // LANES, LANES)
    a = a.transpose(*range(k), k, k + 2, k + 1, k + 3)
    return a.reshape(*lead, cols // ROWS, lats // LANES * ROWS, LANES)


def from_tiles(a, cols, lats):
    *lead, _, _, _ = a.shape
    k = len(lead)
    a = a.reshape(*lead, cols // ROWS, lats // LANES, ROWS, LANES)
    a = a.transpose(*range(k), k, k + 2, k + 1, k + 3)
    return a.reshape(*lead, cols, lats)


def in_hbm(a):
    return pltpu.with_memory_space_constraint(a, pltpu.HBM)


def on_device(n, tracer, offsets, frac, air_before, air_after, growth):
    S, L, W, lats = tracer.shape
    tiles = to_tiles(tracer)
    f32, vmem = jnp.float32, pltpu.VMEM
    column = (ROWS, LANES)
    blocks = W // ROWS
    dma = pltpu.SemaphoreType.DMA
    reach = n // 8
    rounds = len(know_steps(1, 2 * reach + 1))
    small = (L, blocks, ROWS * ROWS, LANES)
    limited, factor = pl.pallas_call(
        functools.partial(kernel, (S, L, W, n)),
        out_shape=[pltpu.VMEM(tiles.shape, f32), pltpu.VMEM((S, *column), f32)],
        in_specs=[pl.BlockSpec(memory_space=pltpu.HBM)] * 6,

        out_specs=[pl.BlockSpec(memory_space=pltpu.VMEM)] * 2,
        scratch_shapes=[
            vmem(tiles.shape, f32),
            vmem((2, L, ROWS * ROWS, LANES), f32),
            vmem(frac.shape, f32),
            pltpu.SMEM(growth.shape, f32),
            vmem(small, jnp.int32),
            vmem(small, f32),
            vmem(small, f32),
            vmem((S, L, LOW + W + HIGH, *column), f32),
            vmem((L, W, *column), jnp.int32),
            vmem((L, W, *column), f32),
            vmem((L, W, *column), f32),
            vmem((L, W, *column), f32),
            vmem((L, OFFMAX, *column), f32),
            vmem((L, OFFMAX + 1, *column), f32),
            vmem((L, OFFMAX + 1, *column), f32),
            vmem((L, OFFMAX, *column), f32),
            vmem((S, L, W + 2 * OFFMAX, *column), f32),
            vmem((4, L, *column), f32),
            vmem((2 * S, *column), f32),
            vmem((1, LANES), f32),
            vmem((1, LANES), f32),
            vmem((1, LANES), f32),
            vmem((reach, 1, LANES), f32),
            vmem((1, LANES), f32),
            vmem((1, LANES), f32),
            vmem((1, LANES), f32),
            vmem((2, 1, LANES), f32),
            dma((2,)),
            dma((S,)),
            dma((5,)),
            dma((2,)),
            dma((2,)),
            dma((4,)),
            dma((4,)),
            dma((2,)),
            dma((2,)),
            dma((2, S - 1 + L)),
            dma((2, S - 1 + L)),
            pltpu.SemaphoreType.REGULAR((rounds, 2)),
            dma((2,)),
            dma((2,)),
            dma((reach,)),
            dma((reach,)),
            dma((2,)),
            dma((2,)),
        ],
        compiler_params=pltpu.CompilerParams(collective_id=0, has_side_effects=True, vmem_limit_bytes=44 * 2**20),
    )(*map(in_hbm, (tiles, to_tiles(offsets), to_tiles(air_before), to_tiles(air_after), frac, growth)))
    result = pl.pallas_call(
        scale_kernel,
        out_shape=jax.ShapeDtypeStruct(tiles.shape, f32),
        in_specs=[pl.BlockSpec(memory_space=pltpu.VMEM)] * 2,
        out_specs=pl.BlockSpec(memory_space=pl.ANY),
        scratch_shapes=[vmem(tiles.shape, f32), dma((S,))],
        compiler_params=pltpu.CompilerParams(vmem_limit_bytes=24 * 2**20),
    )(limited, factor)
    return from_tiles(result, W, lats)


def solution(mesh):
    placed = (
        P("scen", None, "lon", None),
        P(None, "lon", None),
        P(),
        P(None, "lon", None),
        P(None, "lon", None),
        P("scen"),
    )
    return jax.shard_map(
        functools.partial(on_device, mesh.shape["lon"]),
        mesh=mesh,
        in_specs=placed,
        out_specs=P("scen", None, "lon", None),
        check_vma=False,
    )
```

```python
import functools

import jax
import jax.numpy as jnp
from jax import lax
from jax.experimental import pallas as pl
from jax.experimental.pallas import tpu as pltpu
from jax.sharding import PartitionSpec as P

OFFMAX = 12
LANES = 128
ROWS = 8
LOW = OFFMAX + 1
HIGH = OFFMAX + 2
MESH = pl.DeviceIdType.MESH


def know_steps(known, wanted):
    steps = []
    while known < wanted:
        steps.append(min(known, wanted - known))
        known += steps[-1]
    return steps


def cubic_weights(fraction):
    first = -fraction * (1.0 - fraction) * (2.0 - fraction) / 6.0
    second = (1.0 + fraction) * (1.0 - fraction) * (2.0 - fraction) / 2.0
    third = (1.0 + fraction) * fraction * (2.0 - fraction) / 2.0
    fourth = -(1.0 + fraction) * fraction * (1.0 - fraction) / 6.0
    return (first, second, third, fourth)


def pick(bits, items):
    for bit in bits:
        merged = [jnp.where(bit, items[j + 1], items[j]) for j in range(0, len(items) - 1, 2)]
        if len(items) % 2:
            merged.append(items[-1])
        items = merged
    return items[0]


def kernel(
    dims,
    tracer,
    offsets,
    air_before,
    air_after,
    frac,
    growth,
    out,
    t_in,
    t_halo,
    frac_in,
    growth_in,
    off_in,
    ab_in,
    aa_in,
    t_col,
    k_col,
    ab_col,
    aa_col,
    g_col,
    g_out_down,
    g_out_up,
    g_low,
    g_high,
    f_col,
    weight,
    acc,
    factor,
    row_own,
    row_pair,
    row_chip,
    rows_near,
    row_side,
    row_other,
    row_far_out,
    rows_far,
    edge_in_sem,
    in_sem,
    small_in_sem,
    tile_send,
    tile_recv,
    edge_send,
    edge_recv,
    g_send,
    g_recv,
    bulk_send,
    bulk_recv,
    know,
    pair_send,
    pair_recv,
    near_send,
    near_recv,
    far_send,
    far_recv,
):
    S, L, W, n = dims
    blocks = W // ROWS
    reach = n // 8
    me = lax.axis_index("lon")
    core = lax.rem(me, 2)
    left, right = lax.rem(me + n - 1, n), lax.rem(me + 1, n)
    partner = me + 1 - 2 * core

    def away(distance):
        return lax.rem(me + distance + n, n)

    barrier = pltpu.get_barrier_semaphore()
    for to in (left, right):
        pl.semaphore_signal(barrier, inc=1, device_id={"lon": to}, device_id_type=MESH)

    load_edges = [
        pltpu.make_async_copy(tracer.at[:, :, blk], t_in.at[:, :, blk], edge_in_sem.at[i])
        for i, blk in enumerate((0, blocks - 1))
    ]
    load_off = pltpu.make_async_copy(offsets, off_in, small_in_sem.at[0])
    load_aa = pltpu.make_async_copy(air_after, aa_in, small_in_sem.at[1])
    load_ab = pltpu.make_async_copy(air_before, ab_in, small_in_sem.at[2])
    load_frac = pltpu.make_async_copy(frac, frac_in, small_in_sem.at[3])
    load_growth = pltpu.make_async_copy(growth, growth_in, small_in_sem.at[4])

    def load_inner(s):
        inner = pl.ds(1, blocks - 2)
        return pltpu.make_async_copy(tracer.at[s, :, inner], t_in.at[s, :, inner], in_sem.at[s])

    for copy in (*load_edges, load_off, load_aa, load_frac, load_ab, load_growth):
        copy.start()
    for s in range(S):
        load_inner(s).start()

    def remote(src, dst, send, recv, to):
        return pltpu.make_async_remote_copy(
            src_ref=src, dst_ref=dst, send_sem=send, recv_sem=recv, device_id={"lon": to}, device_id_type=MESH
        )

    tile_up = remote(tracer.at[0, :, blocks - 1], t_halo.at[0], tile_send.at[0], tile_recv.at[0], right)
    tile_down = remote(tracer.at[0, :, 0], t_halo.at[1], tile_send.at[1], tile_recv.at[1], left)
    half = S // 2

    def edge(species, count, source, target, sem, to):
        return remote(
            t_col.at[species, :, pl.ds(source, count)], t_col.at[species, :, pl.ds(target, count)], edge_send.at[sem], edge_recv.at[sem], to
        )

    one_half, other_half = pl.ds(1, half - 1), pl.ds(half, S - half)
    edges = [
        edge(one_half, 2, LOW, LOW + W, 0, left),
        edge(one_half, 1, LOW + W - 1, LOW - 1, 1, right),
        edge(other_half, 2, LOW + W - 2, LOW - 2, 2, right),
        edge(other_half, 1, LOW, LOW + W, 3, left),
    ]
    g_down = remote(g_out_down, g_high, g_send.at[0], g_recv.at[0], left)
    g_up = remote(g_out_up, g_low, g_send.at[1], g_recv.at[1], right)

    def bulk(s, sem, levels, up_count, down_first):
        down_count = HIGH - down_first
        return (
            remote(
                t_col.at[s, levels, pl.ds(W, up_count)],
                t_col.at[s, levels, pl.ds(0, up_count)],
                bulk_send.at[0, sem],
                bulk_recv.at[0, sem],
                right,
            ),
            remote(
                t_col.at[s, levels, pl.ds(LOW + down_first, down_count)],
                t_col.at[s, levels, pl.ds(LOW + W + down_first, down_count)],
                bulk_send.at[1, sem],
                bulk_recv.at[1, sem],
                left,
            ),
        )

    def bulk_first():
        return bulk(0, 0, pl.ds(0, L), LOW - ROWS, ROWS)

    def bulk_one(s):
        return bulk(s, s, pl.ds(0, L), LOW - 1, 2)

    def bulk_other(s):
        return bulk(s, s, pl.ds(0, L), LOW - 2, 1)

    def bulk_last(lev):
        return bulk(S - 1, S - 1 + lev, pl.ds(lev, 1), LOW - 2, 1)

    steps = know_steps(1, 2 * reach + 1)
    rounds = len(steps)

    def tell(r):
        if r >= rounds:
            return
        for side, distance in ((0, steps[r]), (1, -steps[r])):
            pl.semaphore_signal(know.at[r, side], inc=1, device_id={"lon": away(distance)}, device_id_type=MESH)

    def hear(r):
        if r >= rounds:
            return
        for side in range(2):
            pl.semaphore_wait(know.at[r, side], 1)

    pl.semaphore_wait(barrier, 2)
    tile_up.start()
    tile_down.start()
    tell(0)

    for copy in load_edges:
        copy.wait()

    def relay_edges(s, _):
        for lev in range(L):
            for blk, l in ((0, 0), (0, 1), (blocks - 1, ROWS - 2), (blocks - 1, ROWS - 1)):
                t_col[s, lev, LOW + blk * ROWS + l] = t_in[s, lev, blk, pl.ds(l, ROWS, stride=ROWS), :]
        return 0

    lax.fori_loop(0, S, relay_edges, 0)
    for copy in edges:
        copy.start()
    hear(0)
    tell(1)
    load_off.wait()
    load_aa.wait()

    def relay_small(x, _):
        lev, blk = x // blocks, lax.rem(x, blocks)
        for l in range(ROWS):
            k_col[lev, blk * ROWS + l] = OFFMAX - off_in[lev, blk, pl.ds(l, ROWS, stride=ROWS), :]
            aa_col[lev, blk * ROWS + l] = aa_in[lev, blk, pl.ds(l, ROWS, stride=ROWS), :]
        return 0

    lax.fori_loop(0, L * blocks, relay_small, 0)

    def weight_of(lev, b):
        total = None
        for i in range(max(0, b - OFFMAX), min(W - 1, b + OFFMAX) + 1):
            term = jnp.where(k_col[lev, i] == OFFMAX - i + b, aa_col[lev, i], 0.0)
            total = term if total is None else total + term
        return total

    def g_sides(lev, _):
        for j in range(OFFMAX):
            g_out_down[lev, j] = weight_of(lev, j - OFFMAX)
        for j in range(OFFMAX + 1):
            g_out_up[lev, j] = weight_of(lev, W - 1 + j)
        return 0

    lax.fori_loop(0, L, g_sides, 0)
    load_frac.wait()
    for lev in range(L):
        for j in range(ROWS):
            weight[0, lev, j : j + 1, :] = frac_in[lev : lev + 1, j * LANES : (j + 1) * LANES]
        for tap, w in enumerate(cubic_weights(weight[0, lev])):
            weight[tap, lev] = w
    g_down.start()
    g_up.start()
    load_ab.wait()

    def relay_before(x, _):
        lev, blk = x // blocks, lax.rem(x, blocks)
        for l in range(ROWS):
            ab_col[lev, blk * ROWS + l] = ab_in[lev, blk, pl.ds(l, ROWS, stride=ROWS), :]
        return 0

    lax.fori_loop(0, L * blocks, relay_before, 0)

    zero = jnp.zeros((ROWS, LANES), jnp.float32)

    def relay_species(s, _):
        load_inner(s).wait()

        def relay(lev, totals):
            totals = list(totals)
            for i in range(W):
                blk, l = divmod(i, ROWS)
                if 2 <= i < W - 2:
                    value = t_in[s, lev, blk, pl.ds(l, ROWS, stride=ROWS), :]
                    t_col[s, lev, LOW + i] = value
                else:
                    value = t_col[s, lev, LOW + i]
                totals[i % 4] = totals[i % 4] + value * ab_col[lev, i]
            return tuple(totals)

        totals = lax.fori_loop(0, L, relay, (zero,) * 4)
        acc[s] = (totals[0] + totals[1]) + (totals[2] + totals[3])
        return 0

    lax.fori_loop(0, half, relay_species, 0)
    hear(1)
    tell(2)
    lax.fori_loop(half, S, relay_species, 0)
    for copy in bulk_first():
        copy.start()

    def send_one(s, _):
        for copy in bulk_one(s):
            copy.start()
        return 0

    def send_other(s, _):
        for copy in bulk_other(s):
            copy.start()
        return 0

    lax.fori_loop(1, half, send_one, 0)
    lax.fori_loop(half, S - 1, send_other, 0)
    for lev in range(L):
        for copy in bulk_last(lev):
            copy.start()

    def g_inside(lev, _):
        for b in range(W - 1):
            g_col[lev, b] = weight_of(lev, b)
        g_col[lev, W - 1] = g_out_up[lev, 0]
        return 0

    lax.fori_loop(0, L, g_inside, 0)
    hear(2)
    tell(3)

    def departures(s, lev, first, count):
        w = [weight[tap, lev] for tap in range(4)]
        t = [t_col[s, lev, LOW + first - 1 + j] for j in range(count + 3)]
        values = []
        for j in range(count):
            cubic = w[0] * t[j] + w[1] * t[j + 1]
            cubic = cubic + w[2] * t[j + 2] + w[3] * t[j + 3]
            low, high = jnp.minimum(t[j + 1], t[j + 2]), jnp.maximum(t[j + 1], t[j + 2])
            values.append(jnp.minimum(jnp.maximum(cubic, low), high))
            f_col[s, lev, OFFMAX + first + j] = values[-1]
        return values

    def inside(s, _):
        def level(lev, totals):
            totals = list(totals)
            for first in range(1, W - 2, ROWS):
                for j, value in enumerate(departures(s, lev, first, min(ROWS, W - 2 - first))):
                    totals[j % 4] = totals[j % 4] + value * g_col[lev, first + j]
            return tuple(totals)

        totals = lax.fori_loop(0, L, level, (zero,) * 4)
        acc[S + s] = (totals[0] + totals[1]) + (totals[2] + totals[3])
        return 0

    lax.fori_loop(0, S, inside, 0)
    hear(3)
    tell(4)

    tile_up.wait_recv()
    tile_down.wait_recv()

    def relay_tiles(lev, _):
        for l in range(ROWS):
            rows = pl.ds(l, ROWS, stride=ROWS)
            t_col[0, lev, LOW - ROWS + l] = t_halo[0, lev, rows, :]
            t_col[0, lev, LOW + W + l] = t_halo[1, lev, rows, :]
        return 0

    lax.fori_loop(0, L, relay_tiles, 0)
    for copy in edges:
        copy.wait_recv()
    g_down.wait_recv()
    g_up.wait_recv()

    def outer_mass(lev, totals):
        low = [g_low[lev, j] for j in range(OFFMAX + 1)]
        high = [g_high[lev, j] for j in range(OFFMAX)]
        low[0] = low[0] + g_out_down[lev, OFFMAX - 1]
        low[1] = low[1] + g_col[lev, 0]
        high[OFFMAX - 2] = high[OFFMAX - 2] + g_col[lev, W - 2]
        high[OFFMAX - 1] = high[OFFMAX - 1] + g_col[lev, W - 1]
        sums = []
        for s in range(S):
            parts = [totals[s], zero]
            if s < half:
                first, last = departures(s, lev, 0, 1), departures(s, lev, W - 2, 2)
            else:
                first, last = departures(s, lev, -1, 2), departures(s, lev, W - 2, 1)
            near_low = [(first[-1], low[1])] + [(f_col[s, lev, OFFMAX + j], low[1 + j]) for j in range(1, OFFMAX)]
            if s >= half:
                near_low.append((first[0], low[0]))
            near_high = [(f_col[s, lev, W + j], high[j]) for j in range(OFFMAX - 2)]
            near_high += [(value, high[OFFMAX - 2 + j]) for j, value in enumerate(last)]
            for i, pairs in enumerate((near_low, near_high)):
                for value, mass in pairs:
                    parts[i] = parts[i] + value * mass
            sums.append(parts[0] + parts[1])
        return tuple(sums)

    totals = lax.fori_loop(0, L, outer_mass, tuple(acc[S + s] for s in range(S)))
    for s in range(S):
        acc[S + s] = totals[s]

    sums = jnp.sum(jnp.sum(acc[...], axis=1), axis=1, keepdims=True)
    at_row = lax.broadcasted_iota(jnp.int32, (2 * S, LANES), 0)
    at_lane = lax.broadcasted_iota(jnp.int32, (2 * S, LANES), 1)
    row_own[...] = jnp.sum(jnp.where(at_row == at_lane, sums, 0.0), axis=0, keepdims=True)

    pair = remote(row_own, row_pair, pair_send.at[0], pair_recv.at[0], partner)
    pair.start()
    pair.wait_recv()
    row_chip[...] = row_own[...] + row_pair[...]
    for r in range(4, rounds):
        hear(r)
        tell(r + 1)

    way = 2 * (1 - 2 * core)
    near = [remote(row_chip, rows_near.at[d], near_send.at[d], near_recv.at[d], away(way * (d + 1))) for d in range(reach)]

    @pl.when(core == 1)
    def _():
        near[reach - 1].start()

    for copy in near[reach - 2 :: -1]:
        copy.start()

    def halo(s, lev):
        for first, count in ((-OFFMAX, 6), (-OFFMAX + 6, 6), (W - 1, 7), (W + 6, 6)):
            departures(s, lev, first, count)

    def gather(s, lev, blk):
        base = blk * ROWS
        f = [f_col[s, lev, base + j] for j in range(ROWS + 2 * OFFMAX)]
        for l in range(ROWS):
            k = k_col[lev, base + l]
            bits = [(k & (1 << bit)) != 0 for bit in range(5)]
            out[s, lev, blk, pl.ds(l, ROWS, stride=ROWS), :] = pick(bits, f[l : l + 2 * OFFMAX + 1])

    def level_cells(s, lev):
        def part(blk, _):
            gather(s, lev, blk)
            return 0

        halo(s, lev)
        lax.fori_loop(0, blocks, part, 0)

    def cells(s, copies):
        for copy in copies:
            copy.wait_recv()

        def level(lev, _):
            level_cells(s, lev)
            return 0

        lax.fori_loop(0, L, level, 0)

    def one_cells(s, _):
        cells(s, bulk_one(s))
        return 0

    def other_cells(s, _):
        cells(s, bulk_other(s))
        return 0

    early = max(1, half - 1)
    cells(0, bulk_first())
    lax.fori_loop(1, early, one_cells, 0)

    for copy in near[:-1]:
        copy.wait_recv()
    mine = jnp.sum(rows_near[pl.ds(0, reach - 1)], axis=0)

    @pl.when(core == 0)
    def _():
        row_far_out[...] = mine + row_chip[...]
        row_side[...] = mine

    @pl.when(core == 1)
    def _():
        near[reach - 1].wait_recv()
        row_far_out[...] = mine + rows_near[reach - 1]
        row_side[...] = mine + rows_near[reach - 1]

    far = [
        remote(row_far_out, rows_far.at[core], far_send.at[at], far_recv.at[core], away(way * reach - core + at)) for at in range(2)
    ]
    for copy in far:
        copy.start()
    swap = remote(row_side, row_other, pair_send.at[1], pair_recv.at[1], partner)
    swap.start()

    lax.fori_loop(early, half, one_cells, 0)
    lax.fori_loop(half, S - 1, other_cells, 0)
    def last_cells(lev):
        for copy in bulk_last(lev):
            copy.wait_recv()
        level_cells(S - 1, lev)

    for lev in range(L - 1):
        last_cells(lev)
    swap.wait_recv()
    for side in range(2):
        remote(row_far_out, rows_far.at[side], far_send.at[0], far_recv.at[side], partner).wait_recv()
    load_growth.wait()
    total = row_chip[...] + (row_side[...] + row_other[...]) + (rows_far[0] + rows_far[1])
    spread = jnp.broadcast_to(total, (S, LANES))
    at_row = lax.broadcasted_iota(jnp.int32, (S, LANES), 0)
    at_lane = lax.broadcasted_iota(jnp.int32, (S, LANES), 1)
    before = jnp.sum(jnp.where(at_lane == at_row, spread, 0.0), axis=1, keepdims=True)
    after = jnp.sum(jnp.where(at_lane == at_row + S, spread, 0.0), axis=1, keepdims=True)
    gain = jnp.zeros((S, LANES), jnp.float32)
    for s in range(S):
        gain = jnp.where(at_row == s, 1.0 + growth_in[s], gain)
    ratio = before * gain / after
    for s in range(S):
        factor[s] = jnp.broadcast_to(ratio[s : s + 1, :], (ROWS, LANES))

    def scale(x, _):
        s, lev = x // L, lax.rem(x, L)
        gain = factor[s]
        for blk in range(blocks):
            for row in range(0, out.shape[3], ROWS):
                out[s, lev, blk, pl.ds(row, ROWS), :] = out[s, lev, blk, pl.ds(row, ROWS), :] * gain
        return 0

    lax.fori_loop(0, S * L - 1, scale, 0)
    last_cells(L - 1)
    scale(S * L - 1, 0)

    for copy in (tile_up, tile_down, *edges, g_down, g_up, pair, swap, *near[:-1], *far, *bulk_first()):
        copy.wait_send()

    @pl.when(core == 1)
    def _():
        near[reach - 1].wait_send()

    for lev in range(L):
        for copy in bulk_last(lev):
            copy.wait_send()

    def finish_one(s, _):
        for copy in bulk_one(s):
            copy.wait_send()
        return 0

    def finish_other(s, _):
        for copy in bulk_other(s):
            copy.wait_send()
        return 0

    lax.fori_loop(1, half, finish_one, 0)
    lax.fori_loop(half, S - 1, finish_other, 0)


def write_kernel(scaled, out, sem):
    def put(s):
        return pltpu.make_async_copy(scaled.at[s], out.at[s], sem.at[s])

    for s in range(out.shape[0]):
        put(s).start()
    for s in range(out.shape[0]):
        put(s).wait()


def to_tiles(a):
    *lead, cols, lats = a.shape
    k = len(lead)
    a = a.reshape(*lead, cols // ROWS, ROWS, lats // LANES, LANES)
    a = a.transpose(*range(k), k, k + 2, k + 1, k + 3)
    return a.reshape(*lead, cols // ROWS, lats // LANES * ROWS, LANES)


def from_tiles(a, cols, lats):
    *lead, _, _, _ = a.shape
    k = len(lead)
    a = a.reshape(*lead, cols // ROWS, lats // LANES, ROWS, LANES)
    a = a.transpose(*range(k), k, k + 2, k + 1, k + 3)
    return a.reshape(*lead, cols, lats)


def in_hbm(a):
    return pltpu.with_memory_space_constraint(a, pltpu.HBM)


def on_device(n, tracer, offsets, frac, air_before, air_after, growth):
    S, L, W, lats = tracer.shape
    tiles = to_tiles(tracer)
    f32, vmem = jnp.float32, pltpu.VMEM
    column = (ROWS, LANES)
    blocks = W // ROWS
    dma = pltpu.SemaphoreType.DMA
    reach = n // 8
    rounds = len(know_steps(1, 2 * reach + 1))
    small = (L, blocks, ROWS * ROWS, LANES)
    scaled = pl.pallas_call(
        functools.partial(kernel, (S, L, W, n)),
        out_shape=pltpu.VMEM(tiles.shape, f32),
        in_specs=[pl.BlockSpec(memory_space=pltpu.HBM)] * 6,

        out_specs=pl.BlockSpec(memory_space=pltpu.VMEM),
        scratch_shapes=[
            vmem(tiles.shape, f32),
            vmem((2, L, ROWS * ROWS, LANES), f32),
            vmem(frac.shape, f32),
            pltpu.SMEM(growth.shape, f32),
            vmem(small, jnp.int32),
            vmem(small, f32),
            vmem(small, f32),
            vmem((S, L, LOW + W + HIGH, *column), f32),
            vmem((L, W, *column), jnp.int32),
            vmem((L, W, *column), f32),
            vmem((L, W, *column), f32),
            vmem((L, W, *column), f32),
            vmem((L, OFFMAX, *column), f32),
            vmem((L, OFFMAX + 1, *column), f32),
            vmem((L, OFFMAX + 1, *column), f32),
            vmem((L, OFFMAX, *column), f32),
            vmem((S, L, W + 2 * OFFMAX, *column), f32),
            vmem((4, L, *column), f32),
            vmem((2 * S, *column), f32),
            vmem((S, *column), f32),
            vmem((1, LANES), f32),
            vmem((1, LANES), f32),
            vmem((1, LANES), f32),
            vmem((reach, 1, LANES), f32),
            vmem((1, LANES), f32),
            vmem((1, LANES), f32),
            vmem((1, LANES), f32),
            vmem((2, 1, LANES), f32),
            dma((2,)),
            dma((S,)),
            dma((5,)),
            dma((2,)),
            dma((2,)),
            dma((4,)),
            dma((4,)),
            dma((2,)),
            dma((2,)),
            dma((2, S - 1 + L)),
            dma((2, S - 1 + L)),
            pltpu.SemaphoreType.REGULAR((rounds, 2)),
            dma((2,)),
            dma((2,)),
            dma((reach,)),
            dma((reach,)),
            dma((2,)),
            dma((2,)),
        ],
        compiler_params=pltpu.CompilerParams(collective_id=0, has_side_effects=True, vmem_limit_bytes=44 * 2**20),
    )(*map(in_hbm, (tiles, to_tiles(offsets), to_tiles(air_before), to_tiles(air_after), frac, growth)))
    result = pl.pallas_call(
        write_kernel,
        out_shape=jax.ShapeDtypeStruct(tiles.shape, f32),
        in_specs=[pl.BlockSpec(memory_space=pltpu.VMEM)],
        out_specs=pl.BlockSpec(memory_space=pl.ANY),
        scratch_shapes=[dma((S,))],
        compiler_params=pltpu.CompilerParams(vmem_limit_bytes=24 * 2**20),
    )(scaled)
    return from_tiles(result, W, lats)


def solution(mesh):
    placed = (
        P("scen", None, "lon", None),
        P(None, "lon", None),
        P(),
        P(None, "lon", None),
        P(None, "lon", None),
        P("scen"),
    )
    return jax.shard_map(
        functools.partial(on_device, mesh.shape["lon"]),
        mesh=mesh,
        in_specs=placed,
        out_specs=P("scen", None, "lon", None),
        check_vma=False,
    )
```

```python
import functools

import jax
import jax.numpy as jnp
from jax import lax
from jax.experimental import pallas as pl
from jax.experimental.pallas import tpu as pltpu
from jax.sharding import PartitionSpec as P

OFFMAX = 12
LANES = 128
ROWS = 8
LOW = OFFMAX + 1
HIGH = OFFMAX + 2
MESH = pl.DeviceIdType.MESH


def know_steps(known, wanted):
    steps = []
    while known < wanted:
        steps.append(min(known, wanted - known))
        known += steps[-1]
    return steps


def cubic_weights(fraction):
    first = -fraction * (1.0 - fraction) * (2.0 - fraction) / 6.0
    second = (1.0 + fraction) * (1.0 - fraction) * (2.0 - fraction) / 2.0
    third = (1.0 + fraction) * fraction * (2.0 - fraction) / 2.0
    fourth = -(1.0 + fraction) * fraction * (1.0 - fraction) / 6.0
    return (first, second, third, fourth)


def pick(bits, items):
    for bit in bits:
        merged = [jnp.where(bit, items[j + 1], items[j]) for j in range(0, len(items) - 1, 2)]
        if len(items) % 2:
            merged.append(items[-1])
        items = merged
    return items[0]


def kernel(
    dims,
    tracer,
    offsets,
    air_before,
    air_after,
    frac,
    growth,
    out,
    factor,
    t_in,
    t_halo,
    frac_in,
    growth_in,
    off_in,
    ab_in,
    aa_in,
    t_col,
    k_col,
    ab_col,
    aa_col,
    g_col,
    g_out_down,
    g_out_up,
    g_low,
    g_high,
    f_col,
    weight,
    acc,
    row_own,
    row_pair,
    row_chip,
    rows_near,
    row_side,
    row_other,
    row_far_out,
    rows_far,
    edge_in_sem,
    in_sem,
    small_in_sem,
    tile_send,
    tile_recv,
    edge_send,
    edge_recv,
    g_send,
    g_recv,
    bulk_send,
    bulk_recv,
    know,
    pair_send,
    pair_recv,
    near_send,
    near_recv,
    far_send,
    far_recv,
):
    S, L, W, n = dims
    blocks = W // ROWS
    reach = n // 8
    me = lax.axis_index("lon")
    core = lax.rem(me, 2)
    left, right = lax.rem(me + n - 1, n), lax.rem(me + 1, n)
    partner = me + 1 - 2 * core

    def away(distance):
        return lax.rem(me + distance + n, n)

    barrier = pltpu.get_barrier_semaphore()
    for to in (left, right):
        pl.semaphore_signal(barrier, inc=1, device_id={"lon": to}, device_id_type=MESH)

    load_edges = [
        pltpu.make_async_copy(tracer.at[:, :, blk], t_in.at[:, :, blk], edge_in_sem.at[i])
        for i, blk in enumerate((0, blocks - 1))
    ]
    load_off = pltpu.make_async_copy(offsets, off_in, small_in_sem.at[0])
    load_aa = pltpu.make_async_copy(air_after, aa_in, small_in_sem.at[1])
    load_ab = pltpu.make_async_copy(air_before, ab_in, small_in_sem.at[2])
    load_frac = pltpu.make_async_copy(frac, frac_in, small_in_sem.at[3])
    load_growth = pltpu.make_async_copy(growth, growth_in, small_in_sem.at[4])

    def load_inner(s):
        inner = pl.ds(1, blocks - 2)
        return pltpu.make_async_copy(tracer.at[s, :, inner], t_in.at[s, :, inner], in_sem.at[s])

    for copy in (*load_edges, load_off, load_aa, load_frac, load_ab, load_growth):
        copy.start()
    for s in range(S):
        load_inner(s).start()

    def remote(src, dst, send, recv, to):
        return pltpu.make_async_remote_copy(
            src_ref=src, dst_ref=dst, send_sem=send, recv_sem=recv, device_id={"lon": to}, device_id_type=MESH
        )

    tile_up = remote(tracer.at[0, :, blocks - 1], t_halo.at[0], tile_send.at[0], tile_recv.at[0], right)
    tile_down = remote(tracer.at[0, :, 0], t_halo.at[1], tile_send.at[1], tile_recv.at[1], left)
    half = S // 2

    def edge(species, count, source, target, sem, to):
        return remote(
            t_col.at[species, :, pl.ds(source, count)], t_col.at[species, :, pl.ds(target, count)], edge_send.at[sem], edge_recv.at[sem], to
        )

    one_half, other_half = pl.ds(1, half - 1), pl.ds(half, S - half)
    edges = [
        edge(one_half, 2, LOW, LOW + W, 0, left),
        edge(one_half, 1, LOW + W - 1, LOW - 1, 1, right),
        edge(other_half, 2, LOW + W - 2, LOW - 2, 2, right),
        edge(other_half, 1, LOW, LOW + W, 3, left),
    ]
    g_down = remote(g_out_down, g_high, g_send.at[0], g_recv.at[0], left)
    g_up = remote(g_out_up, g_low, g_send.at[1], g_recv.at[1], right)

    def bulk(s, sem, levels, up_count, down_first):
        down_count = HIGH - down_first
        return (
            remote(
                t_col.at[s, levels, pl.ds(W, up_count)],
                t_col.at[s, levels, pl.ds(0, up_count)],
                bulk_send.at[0, sem],
                bulk_recv.at[0, sem],
                right,
            ),
            remote(
                t_col.at[s, levels, pl.ds(LOW + down_first, down_count)],
                t_col.at[s, levels, pl.ds(LOW + W + down_first, down_count)],
                bulk_send.at[1, sem],
                bulk_recv.at[1, sem],
                left,
            ),
        )

    def bulk_first():
        return bulk(0, 0, pl.ds(0, L), LOW - ROWS, ROWS)

    def bulk_one(s):
        return bulk(s, s, pl.ds(0, L), LOW - 1, 2)

    def bulk_other(s):
        return bulk(s, s, pl.ds(0, L), LOW - 2, 1)

    def bulk_last(lev):
        return bulk(S - 1, S - 1 + lev, pl.ds(lev, 1), LOW - 2, 1)

    steps = know_steps(1, 2 * reach + 1)
    rounds = len(steps)

    def tell(r):
        if r >= rounds:
            return
        for side, distance in ((0, steps[r]), (1, -steps[r])):
            pl.semaphore_signal(know.at[r, side], inc=1, device_id={"lon": away(distance)}, device_id_type=MESH)

    def hear(r):
        if r >= rounds:
            return
        for side in range(2):
            pl.semaphore_wait(know.at[r, side], 1)

    pl.semaphore_wait(barrier, 2)
    tile_up.start()
    tile_down.start()
    tell(0)

    for copy in load_edges:
        copy.wait()

    def relay_edges(s, _):
        for lev in range(L):
            for blk, l in ((0, 0), (0, 1), (blocks - 1, ROWS - 2), (blocks - 1, ROWS - 1)):
                t_col[s, lev, LOW + blk * ROWS + l] = t_in[s, lev, blk, pl.ds(l, ROWS, stride=ROWS), :]
        return 0

    lax.fori_loop(0, S, relay_edges, 0)
    for copy in edges:
        copy.start()
    hear(0)
    tell(1)
    load_off.wait()
    load_aa.wait()

    def relay_small(x, _):
        lev, blk = x // blocks, lax.rem(x, blocks)
        for l in range(ROWS):
            k_col[lev, blk * ROWS + l] = OFFMAX - off_in[lev, blk, pl.ds(l, ROWS, stride=ROWS), :]
            aa_col[lev, blk * ROWS + l] = aa_in[lev, blk, pl.ds(l, ROWS, stride=ROWS), :]
        return 0

    lax.fori_loop(0, L * blocks, relay_small, 0)

    def weight_of(lev, b):
        total = None
        for i in range(max(0, b - OFFMAX), min(W - 1, b + OFFMAX) + 1):
            term = jnp.where(k_col[lev, i] == OFFMAX - i + b, aa_col[lev, i], 0.0)
            total = term if total is None else total + term
        return total

    def g_sides(lev, _):
        for j in range(OFFMAX):
            g_out_down[lev, j] = weight_of(lev, j - OFFMAX)
        for j in range(OFFMAX + 1):
            g_out_up[lev, j] = weight_of(lev, W - 1 + j)
        return 0

    lax.fori_loop(0, L, g_sides, 0)
    load_frac.wait()
    for lev in range(L):
        for j in range(ROWS):
            weight[0, lev, j : j + 1, :] = frac_in[lev : lev + 1, j * LANES : (j + 1) * LANES]
        for tap, w in enumerate(cubic_weights(weight[0, lev])):
            weight[tap, lev] = w
    g_down.start()
    g_up.start()
    load_ab.wait()

    def relay_before(x, _):
        lev, blk = x // blocks, lax.rem(x, blocks)
        for l in range(ROWS):
            ab_col[lev, blk * ROWS + l] = ab_in[lev, blk, pl.ds(l, ROWS, stride=ROWS), :]
        return 0

    lax.fori_loop(0, L * blocks, relay_before, 0)

    zero = jnp.zeros((ROWS, LANES), jnp.float32)

    def relay_species(s, _):
        load_inner(s).wait()

        def relay(lev, totals):
            totals = list(totals)
            for i in range(W):
                blk, l = divmod(i, ROWS)
                if 2 <= i < W - 2:
                    value = t_in[s, lev, blk, pl.ds(l, ROWS, stride=ROWS), :]
                    t_col[s, lev, LOW + i] = value
                else:
                    value = t_col[s, lev, LOW + i]
                totals[i % 4] = totals[i % 4] + value * ab_col[lev, i]
            return tuple(totals)

        totals = lax.fori_loop(0, L, relay, (zero,) * 4)
        acc[s] = (totals[0] + totals[1]) + (totals[2] + totals[3])
        return 0

    lax.fori_loop(0, half, relay_species, 0)
    hear(1)
    tell(2)
    lax.fori_loop(half, S, relay_species, 0)
    for copy in bulk_first():
        copy.start()

    def send_one(s, _):
        for copy in bulk_one(s):
            copy.start()
        return 0

    def send_other(s, _):
        for copy in bulk_other(s):
            copy.start()
        return 0

    lax.fori_loop(1, half, send_one, 0)
    lax.fori_loop(half, S - 1, send_other, 0)
    for lev in range(L):
        for copy in bulk_last(lev):
            copy.start()

    def g_inside(lev, _):
        for b in range(W - 1):
            g_col[lev, b] = weight_of(lev, b)
        g_col[lev, W - 1] = g_out_up[lev, 0]
        return 0

    lax.fori_loop(0, L, g_inside, 0)
    hear(2)
    tell(3)

    def departures(s, lev, first, count):
        w = [weight[tap, lev] for tap in range(4)]
        t = [t_col[s, lev, LOW + first - 1 + j] for j in range(count + 3)]
        values = []
        for j in range(count):
            cubic = w[0] * t[j] + w[1] * t[j + 1]
            cubic = cubic + w[2] * t[j + 2] + w[3] * t[j + 3]
            low, high = jnp.minimum(t[j + 1], t[j + 2]), jnp.maximum(t[j + 1], t[j + 2])
            values.append(jnp.minimum(jnp.maximum(cubic, low), high))
            f_col[s, lev, OFFMAX + first + j] = values[-1]
        return values

    def inside(s, _):
        def level(lev, totals):
            totals = list(totals)
            for first in range(1, W - 2, ROWS):
                for j, value in enumerate(departures(s, lev, first, min(ROWS, W - 2 - first))):
                    totals[j % 4] = totals[j % 4] + value * g_col[lev, first + j]
            return tuple(totals)

        totals = lax.fori_loop(0, L, level, (zero,) * 4)
        acc[S + s] = (totals[0] + totals[1]) + (totals[2] + totals[3])
        return 0

    lax.fori_loop(0, S, inside, 0)
    hear(3)
    tell(4)

    tile_up.wait_recv()
    tile_down.wait_recv()

    def relay_tiles(lev, _):
        for l in range(ROWS):
            rows = pl.ds(l, ROWS, stride=ROWS)
            t_col[0, lev, LOW - ROWS + l] = t_halo[0, lev, rows, :]
            t_col[0, lev, LOW + W + l] = t_halo[1, lev, rows, :]
        return 0

    lax.fori_loop(0, L, relay_tiles, 0)
    for copy in edges:
        copy.wait_recv()
    g_down.wait_recv()
    g_up.wait_recv()

    def outer_mass(lev, totals):
        low = [g_low[lev, j] for j in range(OFFMAX + 1)]
        high = [g_high[lev, j] for j in range(OFFMAX)]
        low[0] = low[0] + g_out_down[lev, OFFMAX - 1]
        low[1] = low[1] + g_col[lev, 0]
        high[OFFMAX - 2] = high[OFFMAX - 2] + g_col[lev, W - 2]
        high[OFFMAX - 1] = high[OFFMAX - 1] + g_col[lev, W - 1]
        sums = []
        for s in range(S):
            parts = [totals[s], zero]
            if s < half:
                first, last = departures(s, lev, 0, 1), departures(s, lev, W - 2, 2)
            else:
                first, last = departures(s, lev, -1, 2), departures(s, lev, W - 2, 1)
            near_low = [(first[-1], low[1])] + [(f_col[s, lev, OFFMAX + j], low[1 + j]) for j in range(1, OFFMAX)]
            if s >= half:
                near_low.append((first[0], low[0]))
            near_high = [(f_col[s, lev, W + j], high[j]) for j in range(OFFMAX - 2)]
            near_high += [(value, high[OFFMAX - 2 + j]) for j, value in enumerate(last)]
            for i, pairs in enumerate((near_low, near_high)):
                for value, mass in pairs:
                    parts[i] = parts[i] + value * mass
            sums.append(parts[0] + parts[1])
        return tuple(sums)

    totals = lax.fori_loop(0, L, outer_mass, tuple(acc[S + s] for s in range(S)))
    for s in range(S):
        acc[S + s] = totals[s]

    sums = jnp.sum(jnp.sum(acc[...], axis=1), axis=1, keepdims=True)
    at_row = lax.broadcasted_iota(jnp.int32, (2 * S, LANES), 0)
    at_lane = lax.broadcasted_iota(jnp.int32, (2 * S, LANES), 1)
    row_own[...] = jnp.sum(jnp.where(at_row == at_lane, sums, 0.0), axis=0, keepdims=True)

    pair = remote(row_own, row_pair, pair_send.at[0], pair_recv.at[0], partner)
    pair.start()
    pair.wait_recv()
    row_chip[...] = row_own[...] + row_pair[...]
    for r in range(4, rounds):
        hear(r)
        tell(r + 1)

    way = 2 * (1 - 2 * core)
    near = [remote(row_chip, rows_near.at[d], near_send.at[d], near_recv.at[d], away(way * (d + 1))) for d in range(reach)]

    @pl.when(core == 1)
    def _():
        near[reach - 1].start()

    for copy in near[reach - 2 :: -1]:
        copy.start()

    def halo(s, lev):
        for first, count in ((-OFFMAX, 6), (-OFFMAX + 6, 6), (W - 1, 7), (W + 6, 6)):
            departures(s, lev, first, count)

    def gather(s, lev, blk):
        base = blk * ROWS
        f = [f_col[s, lev, base + j] for j in range(ROWS + 2 * OFFMAX)]
        for l in range(ROWS):
            k = k_col[lev, base + l]
            bits = [(k & (1 << bit)) != 0 for bit in range(5)]
            out[s, lev, blk, pl.ds(l, ROWS, stride=ROWS), :] = pick(bits, f[l : l + 2 * OFFMAX + 1])

    def level_cells(s, lev):
        def part(blk, _):
            gather(s, lev, blk)
            return 0

        halo(s, lev)
        lax.fori_loop(0, blocks, part, 0)

    def cells(s, copies):
        for copy in copies:
            copy.wait_recv()

        def level(lev, _):
            level_cells(s, lev)
            return 0

        lax.fori_loop(0, L, level, 0)

    def one_cells(s, _):
        cells(s, bulk_one(s))
        return 0

    def other_cells(s, _):
        cells(s, bulk_other(s))
        return 0

    early = max(1, half - 1)
    cells(0, bulk_first())
    lax.fori_loop(1, early, one_cells, 0)

    for copy in near[:-1]:
        copy.wait_recv()
    mine = jnp.sum(rows_near[pl.ds(0, reach - 1)], axis=0)

    @pl.when(core == 0)
    def _():
        row_far_out[...] = mine + row_chip[...]
        row_side[...] = mine

    @pl.when(core == 1)
    def _():
        near[reach - 1].wait_recv()
        row_far_out[...] = mine + rows_near[reach - 1]
        row_side[...] = mine + rows_near[reach - 1]

    far = [
        remote(row_far_out, rows_far.at[core], far_send.at[at], far_recv.at[core], away(way * reach - core + at)) for at in range(2)
    ]
    for copy in far:
        copy.start()
    swap = remote(row_side, row_other, pair_send.at[1], pair_recv.at[1], partner)
    swap.start()

    lax.fori_loop(early, half, one_cells, 0)
    lax.fori_loop(half, S - 1, other_cells, 0)
    def last_cells(lev):
        for copy in bulk_last(lev):
            copy.wait_recv()
        level_cells(S - 1, lev)

    for lev in range(L - 1):
        last_cells(lev)
    swap.wait_recv()
    for side in range(2):
        remote(row_far_out, rows_far.at[side], far_send.at[0], far_recv.at[side], partner).wait_recv()
    load_growth.wait()
    total = row_chip[...] + (row_side[...] + row_other[...]) + (rows_far[0] + rows_far[1])
    spread = jnp.broadcast_to(total, (S, LANES))
    at_row = lax.broadcasted_iota(jnp.int32, (S, LANES), 0)
    at_lane = lax.broadcasted_iota(jnp.int32, (S, LANES), 1)
    before = jnp.sum(jnp.where(at_lane == at_row, spread, 0.0), axis=1, keepdims=True)
    after = jnp.sum(jnp.where(at_lane == at_row + S, spread, 0.0), axis=1, keepdims=True)
    gain = jnp.zeros((S, LANES), jnp.float32)
    for s in range(S):
        gain = jnp.where(at_row == s, 1.0 + growth_in[s], gain)
    ratio = before * gain / after
    for s in range(S):
        factor[s] = jnp.broadcast_to(ratio[s : s + 1, :], (ROWS, LANES))

    last_cells(L - 1)

    for copy in (tile_up, tile_down, *edges, g_down, g_up, pair, swap, *near[:-1], *far, *bulk_first()):
        copy.wait_send()

    @pl.when(core == 1)
    def _():
        near[reach - 1].wait_send()

    for lev in range(L):
        for copy in bulk_last(lev):
            copy.wait_send()

    def finish_one(s, _):
        for copy in bulk_one(s):
            copy.wait_send()
        return 0

    def finish_other(s, _):
        for copy in bulk_other(s):
            copy.wait_send()
        return 0

    lax.fori_loop(1, half, finish_one, 0)
    lax.fori_loop(half, S - 1, finish_other, 0)


def scale_kernel(limited, factor, out, scaled, sem):
    S, L = limited.shape[:2]

    def put(s, lev):
        return pltpu.make_async_copy(scaled.at[s, lev], out.at[s, lev], sem.at[s, lev])

    def scale(x, _):
        s, lev = x // L, lax.rem(x, L)
        gain = factor[s]
        for blk in range(limited.shape[2]):
            for row in range(0, limited.shape[3], ROWS):
                scaled[s, lev, blk, pl.ds(row, ROWS), :] = limited[s, lev, blk, pl.ds(row, ROWS), :] * gain
        put(s, lev).start()
        return 0

    def finish(x, _):
        put(x // L, lax.rem(x, L)).wait()
        return 0

    lax.fori_loop(0, S * L, scale, 0)
    lax.fori_loop(0, S * L, finish, 0)


def to_tiles(a):
    *lead, cols, lats = a.shape
    k = len(lead)
    a = a.reshape(*lead, cols // ROWS, ROWS, lats // LANES, LANES)
    a = a.transpose(*range(k), k, k + 2, k + 1, k + 3)
    return a.reshape(*lead, cols // ROWS, lats // LANES * ROWS, LANES)


def from_tiles(a, cols, lats):
    *lead, _, _, _ = a.shape
    k = len(lead)
    a = a.reshape(*lead, cols // ROWS, lats // LANES, ROWS, LANES)
    a = a.transpose(*range(k), k, k + 2, k + 1, k + 3)
    return a.reshape(*lead, cols, lats)


def in_hbm(a):
    return pltpu.with_memory_space_constraint(a, pltpu.HBM)


def on_device(n, tracer, offsets, frac, air_before, air_after, growth):
    S, L, W, lats = tracer.shape
    tiles = to_tiles(tracer)
    f32, vmem = jnp.float32, pltpu.VMEM
    column = (ROWS, LANES)
    blocks = W // ROWS
    dma = pltpu.SemaphoreType.DMA
    reach = n // 8
    rounds = len(know_steps(1, 2 * reach + 1))
    small = (L, blocks, ROWS * ROWS, LANES)
    limited, factor = pl.pallas_call(
        functools.partial(kernel, (S, L, W, n)),
        out_shape=[pltpu.VMEM(tiles.shape, f32), pltpu.VMEM((S, *column), f32)],
        in_specs=[pl.BlockSpec(memory_space=pltpu.HBM)] * 6,

        out_specs=[pl.BlockSpec(memory_space=pltpu.VMEM)] * 2,
        scratch_shapes=[
            vmem(tiles.shape, f32),
            vmem((2, L, ROWS * ROWS, LANES), f32),
            vmem(frac.shape, f32),
            pltpu.SMEM(growth.shape, f32),
            vmem(small, jnp.int32),
            vmem(small, f32),
            vmem(small, f32),
            vmem((S, L, LOW + W + HIGH, *column), f32),
            vmem((L, W, *column), jnp.int32),
            vmem((L, W, *column), f32),
            vmem((L, W, *column), f32),
            vmem((L, W, *column), f32),
            vmem((L, OFFMAX, *column), f32),
            vmem((L, OFFMAX + 1, *column), f32),
            vmem((L, OFFMAX + 1, *column), f32),
            vmem((L, OFFMAX, *column), f32),
            vmem((S, L, W + 2 * OFFMAX, *column), f32),
            vmem((4, L, *column), f32),
            vmem((2 * S, *column), f32),
            vmem((1, LANES), f32),
            vmem((1, LANES), f32),
            vmem((1, LANES), f32),
            vmem((reach, 1, LANES), f32),
            vmem((1, LANES), f32),
            vmem((1, LANES), f32),
            vmem((1, LANES), f32),
            vmem((2, 1, LANES), f32),
            dma((2,)),
            dma((S,)),
            dma((5,)),
            dma((2,)),
            dma((2,)),
            dma((4,)),
            dma((4,)),
            dma((2,)),
            dma((2,)),
            dma((2, S - 1 + L)),
            dma((2, S - 1 + L)),
            pltpu.SemaphoreType.REGULAR((rounds, 2)),
            dma((2,)),
            dma((2,)),
            dma((reach,)),
            dma((reach,)),
            dma((2,)),
            dma((2,)),
        ],
        compiler_params=pltpu.CompilerParams(collective_id=0, has_side_effects=True, vmem_limit_bytes=44 * 2**20),
    )(*map(in_hbm, (tiles, to_tiles(offsets), to_tiles(air_before), to_tiles(air_after), frac, growth)))
    result = pl.pallas_call(
        scale_kernel,
        out_shape=jax.ShapeDtypeStruct(tiles.shape, f32),
        in_specs=[pl.BlockSpec(memory_space=pltpu.VMEM)] * 2,
        out_specs=pl.BlockSpec(memory_space=pl.ANY),
        scratch_shapes=[vmem(tiles.shape, f32), dma((S, L))],
        compiler_params=pltpu.CompilerParams(vmem_limit_bytes=24 * 2**20),
    )(limited, factor)
    return from_tiles(result, W, lats)


def solution(mesh):
    placed = (
        P("scen", None, "lon", None),
        P(None, "lon", None),
        P(),
        P(None, "lon", None),
        P(None, "lon", None),
        P("scen"),
    )
    return jax.shard_map(
        functools.partial(on_device, mesh.shape["lon"]),
        mesh=mesh,
        in_specs=placed,
        out_specs=P("scen", None, "lon", None),
        check_vma=False,
    )
```
